128 devices in a mesh: sub: 32 (over z, y, core), rve: 4 (over x).
Axes of the slice: x: 4, y: 4, z: 4, core: 2. Of those that a mesh axis runs over, the one named last changes fastest.
Arguments:
- displacement: float32 [3, 32, 8, 8], P(None, 'sub', 'rve'), may hold values from -4 to 4
- load: float32 [3, 32, 8, 8], P(None, 'sub', 'rve'), may hold values from -6 to 6
- home_slot: int32 [16384], P(('sub', 'rve')), may hold values from 0 to 16383, as said below
- micro_state: float32 [7, 3, 216, 16384], P(None, None, None, ('sub', 'rve')), may hold values from -6 to 6
- state_slot: int32 [16384], P(('sub', 'rve')), may hold values from 0 to 16383, as said below
- phases: int32 [216, 16384], P(None, ('sub', 'rve')), may hold values from 0 to 2
- phase_moduli: float32 [2, 3], replicated, may hold values from 0.5 to 8
Outputs:
- new_state: float32 [7, 3, 216, 16384], P(None, None, None, ('sub', 'rve'))
- displaced: float32 [3, 32, 8, 8], P(None, 'sub', 'rve')
- residual: float32 [3, 32, 8, 8], P(None, 'sub', 'rve')
- rel_norm: float32 [], replicated
The draws below stay inside these ranges and needn't reach their ends.
Inputs may be any that keep to these rules, and one draw needn't show every extreme that they name: `home_slot`: A permutation of 0 to 16383. The 128 entries held by device s (devices numbered in sub+rve order) contain, for every device d, exactly one value, d * 128 + s, in an order drawn at random; so each device sends exactly one Gauss point to every device. `state_slot`: A permutation of 0 to 16383 with the same structure: the 128 entries held by device s contain, for every device d, exactly one value, d * 128 + s, in an order drawn at random.
All inputs are finite; a program needn't handle non-finite values.
Results may differ from the reference program's by a relative error of at most 0.0003.
Values sent between devices are 32-bit elements; how exact they have to be, the bound alone decides.
A program may use at most 128 MiB of HBM per device.

```python
import math
import jax
import jax.numpy as jnp
import numpy as np
from jax import lax

R = 6
V = 216
CASES = 7
CG_STEPS = 2
NPH = 3
MX = 8
LY = 2
LZ = 1
GP_DEV = 128
PAIR = 1
GPS = 16384
NX = 8
NY = 8
NZ = 32
N_SUB = 32
N_RVE = 4


def slot_law(key):
    device_count = GPS // GP_DEV
    keys = jax.random.split(key, device_count)
    orders = jax.vmap(lambda single: jax.random.permutation(single, GP_DEV))(keys)
    source = jnp.arange(device_count, dtype=jnp.int32)[:, None]
    target = orders // PAIR
    within = orders % PAIR
    return (target * GP_DEV + source * PAIR + within).reshape(-1).astype(jnp.int32)


def draw_home_slot(key, part):
    return slot_law(jax.random.fold_in(key, 11))


def draw_state_slot(key, part):
    return slot_law(jax.random.fold_in(key, 23))


def plant(array, rng, low, largest):
    longest = array.shape.index(max(array.shape))
    spots = []
    for shift in (0, 1):
        where = [jax.random.randint(jax.random.fold_in(rng, axis), (), 0, length) for axis, length in enumerate(array.shape)]
        where[longest] = (where[longest] + shift) % array.shape[longest]
        spots.append(tuple(where))
    return array.at[spots[0]].set(low).at[spots[1]].set(largest)


def level_of(own_key, extent, shards, low, high):
    def one(position, shards_of):
        draws = jax.random.uniform(jax.random.fold_in(jax.random.fold_in(own_key, 6), position), (shards_of,), jnp.float32, low / len(shards), high / len(shards))
        return jnp.repeat(jnp.exp(draws), extent[position] // shards_of).reshape((-1,) + (1,) * (len(extent) - position - 1))

    level = one(*shards[0])
    for cut in shards[1:]:
        level = level * one(*cut)
    return level


def bell_draw(rng, shape, scale, most, shards=(), kind=jnp.bfloat16):
    entries = jax.random.normal(rng, shape, jnp.float32) * scale
    if len(shards) > 0:
        entries = level_of(rng, shape, shards, -0.22, 0.18) * entries
    return jnp.clip(entries, min=-most, max=most).astype(kind)


def setup_inputs(seed: int = 0) -> dict:
    seeds = jax.random.split(jax.random.key(seed), 8)
    displacement = bell_draw(seeds[0], (3, NZ, NY, NX), 0.3, 4.0, ((1, 32), (2, 4)), jnp.float32)
    load = bell_draw(seeds[1], (3, NZ, NY, NX), 1.0, 6.0, ((1, 32), (2, 4)), jnp.float32)
    home_slot = draw_home_slot(jax.random.fold_in(seeds[7], 71), 0)
    micro_state = bell_draw(seeds[3], (CASES, 3, V, GPS), 0.5, 6.0, ((3, 128),), jnp.float32)
    state_slot = draw_state_slot(jax.random.fold_in(seeds[7], 71), 0)
    phases = plant(jax.random.randint(seeds[5], (V, GPS), 0, NPH), jax.random.fold_in(seeds[5], 1), 0, NPH - 1).astype(jnp.int32)
    phase_moduli = jnp.clip(jnp.exp(jax.random.uniform(seeds[6], (2, NPH), jnp.float32, math.log(0.5), math.log(8.0))), 0.5, 8.0)
    return dict(displacement=displacement, load=load, home_slot=home_slot, micro_state=micro_state, state_slot=state_slot, phases=phases, phase_moduli=phase_moduli)


STAB = 0.1
FLOOR = 1.0
voigt_pairs = ((0, 5, 4), (5, 1, 3), (4, 3, 2))
HIGHEST = lax.Precision.HIGHEST

def shape_tables():
    offset = 0.5 / math.sqrt(3.0)
    places = (0.5 - offset, 0.5 + offset)
    slope_table = np.zeros((8, 8, 3))
    for gauss_point in range(8):
        coords = (places[gauss_point % 2], places[gauss_point // 2 % 2], places[gauss_point // 4])
        for corner in range(8):
            corner_bits = (corner % 2, corner // 2 % 2, corner // 4)
            weights = [coords[direction] if corner_bits[direction] == 1 else 1.0 - coords[direction] for direction in range(3)]
            slopes = [1.0 if corner_bits[direction] == 1 else -1.0 for direction in range(3)]
            slope_table[gauss_point, corner, 0] = slopes[0] * weights[1] * weights[2]
            slope_table[gauss_point, corner, 1] = weights[0] * slopes[1] * weights[2]
            slope_table[gauss_point, corner, 2] = weights[0] * weights[1] * slopes[2]
    strain_table = np.zeros((8, 8, 3, 6))
    strain_table[:, :, 0, 0] = slope_table[:, :, 0]
    strain_table[:, :, 0, 4] = slope_table[:, :, 2]
    strain_table[:, :, 0, 5] = slope_table[:, :, 1]
    strain_table[:, :, 1, 1] = slope_table[:, :, 1]
    strain_table[:, :, 1, 3] = slope_table[:, :, 2]
    strain_table[:, :, 1, 5] = slope_table[:, :, 0]
    strain_table[:, :, 2, 2] = slope_table[:, :, 2]
    strain_table[:, :, 2, 3] = slope_table[:, :, 1]
    strain_table[:, :, 2, 4] = slope_table[:, :, 0]
    outer_table = strain_table[:, :, :, :, None] * strain_table[:, :, :, None, :]
    return (jnp.asarray(strain_table, jnp.float32), jnp.asarray(outer_table, jnp.float32))

def voxel_moduli(phases, phase_moduli):
    batch_size = phases.shape[1]
    onehot = (phases[None, :, :] == jnp.arange(NPH, dtype=jnp.int32)[:, None, None]).astype(jnp.float32)
    lame_first = lax.optimization_barrier(jnp.sum(onehot * phase_moduli[0][:, None, None], axis=0))
    lame_second = lax.optimization_barrier(jnp.sum(onehot * phase_moduli[1][:, None, None], axis=0))
    return (lame_first.reshape(R, R, R, batch_size), lame_second.reshape(R, R, R, batch_size))

def micro_stress(voxel_field, imposed, lame_first, lame_second):
    gradients = [[jnp.roll(voxel_field[:, component], -1, axis=1 + direction) - voxel_field[:, component] for direction in range(3)] for component in range(3)]
    strains = []
    for voigt_index, axis_pair in enumerate(((0, 0), (1, 1), (2, 2), (1, 2), (0, 2), (0, 1))):
        left_axis, right_axis = axis_pair
        applied = imposed[:, voigt_index][:, None, None, None, :]
        if left_axis == right_axis:
            strains.append(gradients[left_axis][left_axis] + applied)
        else:
            strains.append(0.5 * (gradients[left_axis][right_axis] + gradients[right_axis][left_axis] + applied))
    volume_change = strains[0] + strains[1] + strains[2]
    stresses = []
    for voigt_index in range(6):
        shear_part = 2.0 * lame_second * strains[voigt_index]
        if voigt_index < 3:
            stresses.append(lame_first * volume_change + shear_part)
        else:
            stresses.append(shear_part)
    return stresses

def divergence(stresses):
    columns_out = []
    for component in range(3):
        summed = 0.0
        for direction in range(3):
            member = stresses[voigt_pairs[direction][component]]
            summed = summed + (jnp.roll(member, 1, axis=1 + direction) - member)
        columns_out.append(summed)
    return jnp.stack(columns_out, axis=1)

def micro_solve(field, imposed, lame_first, lame_second):
    case_count = field.shape[0]
    voxels = field.shape[2]
    batch_size = field.shape[3]
    voxel_field = field.reshape(case_count, 3, R, R, R, batch_size)
    zero_strain = jnp.zeros_like(imposed)

    def apply_force(values, strain):
        return divergence(micro_stress(values, strain, lame_first, lame_second)) + STAB * values
    remainder = -apply_force(voxel_field, imposed)
    search = remainder
    square_sum = lax.optimization_barrier(jnp.sum(remainder * remainder, axis=(1, 2, 3, 4)))
    for step_number in range(CG_STEPS):
        operator_image = apply_force(search, zero_strain)
        curvature = lax.optimization_barrier(jnp.sum(search * operator_image, axis=(1, 2, 3, 4)))
        step_size = (square_sum / curvature)[:, None, None, None, None, :]
        voxel_field = voxel_field + step_size * search
        remainder = remainder - step_size * operator_image
        next_square = lax.optimization_barrier(jnp.sum(remainder * remainder, axis=(1, 2, 3, 4)))
        search = remainder + (next_square / square_sum)[:, None, None, None, None, :] * search
        square_sum = next_square
    stresses = micro_stress(voxel_field, imposed, lame_first, lame_second)
    averaged = jnp.stack([lax.optimization_barrier(jnp.mean(member, axis=(1, 2, 3))) for member in stresses], axis=1)
    return (voxel_field.reshape(case_count, 3, voxels, batch_size), averaged)

def assemble_global(corner_terms):
    summed = jnp.zeros((3, NZ + 1, NY, NX), jnp.float32)
    for corner in range(8):
        shifted = jnp.roll(jnp.roll(corner_terms[corner], corner // 2 % 2, axis=2), corner % 2, axis=3)
        summed = summed.at[:, corner // 4:corner // 4 + NZ].add(shifted)
    return summed[:, :NZ]

def reference(displacement, load, home_slot, micro_state, state_slot, phases, phase_moduli):
    strain_table, outer_table = shape_tables()
    padded = jnp.concatenate([displacement, jnp.zeros((3, 1, NY, NX), jnp.float32)], axis=1)
    corners = jnp.stack([jnp.roll(jnp.roll(padded[:, corner // 4:corner // 4 + NZ], -(corner // 2 % 2), axis=2), -(corner % 2), axis=3) for corner in range(8)])
    gauss_strain = jnp.einsum('qaim,aizyx->qmzyx', strain_table, corners, precision=HIGHEST)
    macro_strain = gauss_strain.reshape(8, 6, N_SUB, LZ, N_RVE, LY, MX).transpose(1, 2, 4, 3, 5, 6, 0).reshape(6, GPS)
    unit_cases = jnp.broadcast_to(jnp.eye(6, dtype=jnp.float32)[:, :, None], (6, 6, GPS))
    imposed = jnp.concatenate([macro_strain[None], unit_cases], axis=0)
    counting = jnp.arange(GPS, dtype=jnp.int32)
    from_home = jnp.zeros((GPS,), jnp.int32).at[home_slot].set(counting)
    from_state = jnp.zeros((GPS,), jnp.int32).at[state_slot].set(counting)
    imposed_slot = imposed[:, :, from_home]

    def solve_block(block_index):
        offset_rows = block_index * GP_DEV
        chosen = lax.dynamic_slice_in_dim(from_state, offset_rows, GP_DEV)
        start_field = jnp.take(micro_state, chosen, axis=3)
        block_imposed = lax.dynamic_slice_in_dim(imposed_slot, offset_rows, GP_DEV, axis=2)
        block_phases = lax.dynamic_slice_in_dim(phases, offset_rows, GP_DEV, axis=1)
        lame_first, lame_second = voxel_moduli(block_phases, phase_moduli)
        return micro_solve(start_field, block_imposed, lame_first, lame_second)
    fields, averaged = lax.map(solve_block, jnp.arange(N_SUB * N_RVE, dtype=jnp.int32))
    new_state = fields.transpose(1, 2, 3, 0, 4).reshape(CASES, 3, V, GPS)
    averaged = averaged.transpose(1, 2, 0, 3).reshape(CASES, 6, GPS)
    at_home = averaged[:, :, home_slot]
    stress = at_home[0].reshape(6, N_SUB, N_RVE, LZ, LY, MX, 8).transpose(0, 6, 1, 3, 2, 4, 5).reshape(6, 8, NZ, NY, NX)
    tangent = at_home[1:].transpose(1, 0, 2).reshape(6, 6, N_SUB, N_RVE, LZ, LY, MX, 8)
    tangent = tangent.transpose(0, 1, 7, 2, 4, 3, 5, 6).reshape(6, 6, 8, NZ, NY, NX)
    force_corner = 0.125 * jnp.einsum('qaim,mqzyx->aizyx', strain_table, stress, precision=HIGHEST)
    diag_corner = 0.125 * jnp.einsum('qaimn,mnqzyx->aizyx', outer_table, tangent, precision=HIGHEST)
    force_int = assemble_global(force_corner)
    stiff_diag = assemble_global(diag_corner)
    residual = load - force_int
    displaced = displacement + residual / jnp.maximum(stiff_diag, FLOOR)
    rel_norm = jnp.sqrt(jnp.sum(residual * residual) / jnp.sum(load * load))
    return (new_state, displaced, residual, rel_norm)
```

```python
import functools
import math

import jax
import jax.numpy as jnp
import numpy as np
from jax import lax
from jax.experimental import pallas as pl
from jax.experimental.pallas import tpu as pltpu
from jax.sharding import PartitionSpec as P

R = 6
VOX = 216
CASES = 7
STAB = 0.1
FLOOR = 1.0
NDEV = 128
NRVE = 4
NSUB = 32
ROWS = CASES * 3 * VOX
CASE_ROWS = 3 * VOX
CHUNKS = (8, 8, 8, 8, 4)
FIRST = (0, 8, 16, 24, 32)
CHUNK_AT = {0: 0, 1: 1, 3: 2, 4: 3, 6: 4}
CELLS = 36
MESH = pl.DeviceIdType.MESH
F32 = jnp.float32
TERMS = (((0, 0), (2, 4), (1, 5)), ((1, 1), (2, 3), (0, 5)), ((2, 2), (1, 3), (0, 4)))


def tables():
    offset = 0.5 / math.sqrt(3.0)
    places = (0.5 - offset, 0.5 + offset)
    slopes = np.zeros((3, 8, NDEV), np.float32)
    for g in range(NDEV):
        q = g % 8
        at = (places[q % 2], places[q // 2 % 2], places[q // 4])
        for a in range(8):
            bits = (a % 2, a // 2 % 2, a // 4)
            w = [at[k] if bits[k] else 1.0 - at[k] for k in range(3)]
            s = [1.0 if bits[k] else -1.0 for k in range(3)]
            slopes[0, a, g] = s[0] * w[1] * w[2]
            slopes[1, a, g] = w[0] * s[1] * w[2]
            slopes[2, a, g] = w[0] * w[1] * s[2]
    mask = np.zeros((8, NDEV), np.float32)
    pick = np.zeros((8, NDEV), np.int32)
    for n in range(48):
        nz, ny, nx = n // 24, n // 8 % 3, n % 8
        for a in range(8):
            ax, ay, az = a % 2, a // 2 % 2, a // 4
            ly = ny - ay
            if az == nz and 0 <= ly < 2:
                mask[a, n] = 1.0
                pick[a, n] = (ly * 8 + (nx - ax) % 8) * 8
    corner = np.zeros((8, NDEV), np.int32)
    for g in range(NDEV):
        ly, ex = g // 64, g // 8 % 8
        for a in range(8):
            ax, ay, az = a % 2, a // 2 % 2, a // 4
            corner[a, g] = az * 24 + (ly + ay) * 8 + (ex + ax) % 8
    floats = np.concatenate([slopes.reshape(24, NDEV), mask], axis=0)
    ints = np.concatenate([pick, corner], axis=0)
    return floats, ints


def dev(d):
    return (d // NRVE, lax.rem(d, NRVE))


def lanes(x, index):
    return jnp.take_along_axis(x, index, axis=1, mode="promise_in_bounds")


def sublanes(x, index):
    return jnp.take_along_axis(x, index, axis=0, mode="promise_in_bounds")


def spread(row):
    return jnp.broadcast_to(row, (8, NDEV))


def inverse(target):
    column = jnp.broadcast_to(target, (NDEV, NDEV)).T
    lane = lax.broadcasted_iota(jnp.int32, (NDEV, NDEV), 1)
    row = lax.broadcasted_iota(jnp.int32, (NDEV, NDEV), 0)
    return jnp.sum(jnp.where(column == lane, row, 0).astype(F32), axis=0, keepdims=True).astype(jnp.int32)


def kernel(
    disp_ref, load_ref, home_ref, state_slot_ref, moduli_ref, micro_ref, phase_ref, float_ref, int_ref,
    new_ref, displaced_ref, residual_ref, norm_ref,
    xin, ph, send0, send1, send2, send3, send4, recv0, recv1, recv2, recv3, recv4,
    nat, outb, lam, mu, w, p0, p1, ap, sig, sums, av, ret_out, ret_in, dtile, dhalo, ntile, nhalo, nrow, nall,
    in_sem, ph_sem, out_sem, local_sem, send_sem, recv_sem, near_send, near_recv,
):
    sub, rve = lax.axis_index("sub"), lax.axis_index("rve")
    me = sub * NRVE + rve
    sends = (send0, send1, send2, send3, send4)
    recvs = (recv0, recv1, recv2, recv3, recv4)

    barrier = pltpu.get_barrier_semaphore()

    @pl.loop(1, NDEV)
    def _(k):
        pl.semaphore_signal(barrier, inc=1, device_id=dev(lax.rem(me + k, NDEV)), device_id_type=MESH)

    loads = []
    for position in range(CASES):
        case = (position + 1) % CASES
        copy = pltpu.make_async_copy(
            micro_ref.at[pl.ds(case * CASE_ROWS, CASE_ROWS)],
            xin.at[pl.ds(position * CASE_ROWS, CASE_ROWS)],
            in_sem.at[position],
        )
        copy.start()
        loads.append(copy)
    phase_load = pltpu.make_async_copy(phase_ref, ph.at[pl.ds(0, VOX)], ph_sem)
    phase_load.start()

    dtile[...] = jnp.zeros((8, NDEV), F32)
    for i in range(3):
        for y in range(2):
            dtile[i : i + 1, 8 * y : 8 * y + 8] = disp_ref[i, 0, y : y + 1, :]

    home_dev = lax.shift_right_logical(home_ref[...], 7)
    state_index = spread(inverse(lax.shift_right_logical(state_slot_ref[...], 7)))
    home_index = spread(inverse(home_dev))

    def prepare(chunk, row, last):
        base = pl.multiple_of((FIRST[chunk] + row) * NDEV, NDEV)
        parts = []
        for i in range(16):
            if last and i > 7:
                parts.append(jnp.zeros((8, NDEV), F32))
            else:
                block = xin[pl.ds(base + 8 * i, 8), :]
                parts.append(lanes(block, home_index if last and i == 7 else state_index))
        pitch = CHUNKS[chunk]
        sends[chunk][pl.ds(row, NDEV, stride=pitch), :] = jnp.concatenate(parts, axis=0).T

    def prepare_chunk(chunk):
        rows = CHUNKS[chunk]
        if chunk < 4:
            for row in range(rows):
                prepare(chunk, row, False)
        else:
            for row in range(rows):
                prepare(chunk, row, row == rows - 1)

    def send_chunk(chunk):
        rows = CHUNKS[chunk]
        own = pl.ds(pl.multiple_of(me * rows, rows), rows)

        @pl.loop(1, NDEV)
        def _(k):
            d = lax.rem(me + k, NDEV)
            pltpu.make_async_remote_copy(
                src_ref=sends[chunk].at[pl.ds(pl.multiple_of(d * rows, rows), rows)],
                dst_ref=recvs[chunk].at[own],
                send_sem=send_sem.at[chunk],
                recv_sem=recv_sem.at[chunk],
                device_id=dev(d),
                device_id_type=MESH,
            ).start()

        pltpu.make_async_copy(sends[chunk].at[own], recvs[chunk].at[own], local_sem.at[chunk]).start()

    def whole(src, dst, rows, index):
        return pltpu.make_async_remote_copy(
            src_ref=src.at[pl.ds(0, (NDEV - 1) * rows)],
            dst_ref=dst.at[pl.ds(0, (NDEV - 1) * rows)],
            send_sem=send_sem.at[index],
            recv_sem=recv_sem.at[index],
            device_id=dev(lax.rem(me + 1, NDEV)),
            device_id_type=MESH,
        )

    for position in (0, 1):
        loads[position].wait()
    prepare_chunk(0)

    pl.semaphore_wait(barrier, NDEV - 1)

    def near(index, src, dst, dsub, drve):
        to_sub = lax.rem(sub + dsub + NSUB, NSUB)
        to_rve = lax.rem(rve + drve + NRVE, NRVE)
        return pltpu.make_async_remote_copy(
            src_ref=src,
            dst_ref=dst,
            send_sem=near_send.at[index],
            recv_sem=near_recv.at[index],
            device_id=(to_sub, to_rve),
            device_id_type=MESH,
        )

    steps = ((0, 1), (1, 0), (1, 1))
    halo_in = [near(i, dtile, dhalo.at[i], -s, -r) for i, (s, r) in enumerate(steps)]
    for copy in halo_in:
        copy.start()
    send_chunk(0)
    for position in (2, 3):
        loads[position].wait()
    prepare_chunk(1)
    send_chunk(1)
    loads[4].wait()
    prepare_chunk(2)
    send_chunk(2)
    for position in (5, 6):
        loads[position].wait()
    prepare_chunk(3)
    send_chunk(3)

    for copy in halo_in:
        copy.wait()
    lane = lax.broadcasted_iota(jnp.int32, (8, NDEV), 1)
    row8 = lax.broadcasted_iota(jnp.int32, (8, NDEV), 0)
    below = jnp.where(sub < NSUB - 1, 1.0, 0.0).astype(F32)
    extended = dtile[...]
    extended = jnp.where((lane >= 16) & (lane < 24), pltpu.roll(dhalo[0], 16, axis=1), extended)
    extended = jnp.where((lane >= 24) & (lane < 40), pltpu.roll(dhalo[1], 24, axis=1) * below, extended)
    extended = jnp.where((lane >= 40) & (lane < 48), pltpu.roll(dhalo[2], 40, axis=1) * below, extended)
    slope = [jnp.zeros((8, NDEV), F32) for _ in range(3)]
    for a in range(8):
        value = lanes(extended, spread(int_ref[8 + a : 9 + a, :]))
        for k in range(3):
            slope[k] = slope[k] + float_ref[8 * k + a : 8 * k + a + 1, :] * value
    s0, s1, s2 = slope
    strains = [
        s0[0:1], s1[1:2], s2[2:3],
        s2[1:2] + s1[2:3], s2[0:1] + s0[2:3], s1[0:1] + s0[1:2],
    ]
    strain_rows = jnp.zeros((8, NDEV), F32)
    for m in range(6):
        strain_rows = jnp.where(row8 == m, spread(strains[m]), strain_rows)
    xin[pl.ds(ROWS, 8), :] = strain_rows
    prepare_chunk(4)
    send_chunk(4)

    phase_load.wait()
    ph[pl.ds(VOX, 8), :] = jnp.zeros((8, NDEV), jnp.int32)
    inside = row8 < R

    @pl.loop(0, CELLS)
    def _(cell):
        label = ph[pl.ds(cell * R, 8), :]
        for which, out in ((0, lam), (1, mu)):
            value = jnp.where(
                label == 0,
                moduli_ref[which, 0],
                jnp.where(label == 1, moduli_ref[which, 1], moduli_ref[which, 2]),
            )
            out[cell] = jnp.where(inside, value, 0.0)

    av[...] = jnp.zeros((NDEV, NDEV), F32)
    up = jnp.where(row8 < 5, row8 + 1, jnp.where(row8 == 5, 0, row8))
    down = jnp.where(row8 == 0, 5, jnp.where(row8 < 6, row8 - 1, row8))

    def receive(chunk):
        rows = CHUNKS[chunk]
        own = pl.ds(pl.multiple_of(me * rows, rows), rows)
        whole(sends[chunk], recvs[chunk], rows, chunk).wait_recv()
        pltpu.make_async_copy(sends[chunk].at[own], recvs[chunk].at[own], local_sem.at[chunk]).wait()
        for row in range(rows):
            block = recvs[chunk][pl.ds(row, NDEV, stride=rows), :]
            nat[pl.ds((FIRST[chunk] + row) * NDEV, NDEV), :] = block.T

    zero = jnp.zeros((8, NDEV), F32)

    def stress_at(src, a, b, applied):
        following = lax.rem(a + 1, R)
        g = []
        for i in range(3):
            here = src[i * CELLS + a * R + b]
            g.append(
                (
                    src[i * CELLS + following * R + b] - here,
                    src[i * CELLS + a * R + (b + 1) % R] - here,
                    sublanes(here, up) - here,
                )
            )
        eps = [g[0][0], g[1][1], g[2][2], g[1][2] + g[2][1], g[0][2] + g[2][0], g[0][1] + g[1][0]]
        if applied is not None:
            eps = [eps[m] + applied[m] for m in range(6)]
        cell = a * R + b
        first, second = lam[cell], mu[cell]
        volume = first * (eps[0] + eps[1] + eps[2])
        twice = second + second
        stress = [volume + twice * eps[m] for m in range(3)] + [second * eps[m] for m in range(3, 6)]
        return stress, eps

    def stresses(src, applied):
        def body(a, total):
            total = list(total)
            for b in range(R):
                stress, _ = stress_at(src, a, b, applied)
                for m in range(6):
                    sig[m * CELLS + a * R + b] = stress[m]
                    total[m] = total[m] + stress[m]
            return tuple(total)

        return lax.fori_loop(0, R, body, (zero,) * 6)

    voigt = ((0, 5, 4), (5, 1, 3), (4, 3, 2))

    def force_at(src, a, b):
        before = lax.rem(a + R - 1, R)
        cell = a * R + b
        here = [sig[m * CELLS + cell] for m in range(6)]
        out = []
        for i in range(3):
            total = sig[voigt[0][i] * CELLS + before * R + b] - here[voigt[0][i]]
            total = total + (sig[voigt[1][i] * CELLS + a * R + (b + R - 1) % R] - here[voigt[1][i]])
            last = here[voigt[2][i]]
            total = total + (sublanes(last, down) - last)
            out.append(total + STAB * src[i * CELLS + cell])
        return out

    def across(x):
        return spread(jnp.sum(x, axis=0, keepdims=True))

    def case_body(position, carry):
        for when, chunk in CHUNK_AT.items():

            @pl.when(position == when)
            def _():
                receive(chunk)

        case = lax.rem(position + 1, CASES)
        macro = nat[pl.ds(ROWS, 8), :]
        applied = []
        for m in range(6):
            unit = jnp.where(position == m, 1.0, 0.0).astype(F32)
            applied.append(jnp.where(position == CASES - 1, spread(macro[m : m + 1, :]), unit))

        @pl.loop(0, CELLS)
        def _(cell):
            for i in range(3):
                at = position * CASE_ROWS + i * VOX + cell * R
                w[i * CELLS + cell] = jnp.where(inside, nat[pl.ds(at, 8), :], 0.0)

        total0 = stresses(w, applied)

        def first(a, rr):
            for b in range(R):
                force = force_at(w, a, b)
                for i in range(3):
                    value = -force[i]
                    p0[i * CELLS + a * R + b] = value
                    rr = rr + value * value
            return rr

        rr = across(lax.fori_loop(0, R, first, zero))
        total1 = stresses(p0, None)

        def second(a, curve):
            for b in range(R):
                force = force_at(p0, a, b)
                for i in range(3):
                    ap[i * CELLS + a * R + b] = force[i]
                    curve = curve + p0[i * CELLS + a * R + b] * force[i]
            return curve

        alpha0 = rr / across(lax.fori_loop(0, R, second, zero))

        def reduce(a, total):
            for j in range(3 * R):
                at = a * (3 * R) + j
                value = p0[at] - alpha0 * ap[at]
                p1[at] = value
                total = total + value * value
            return total

        rn = across(lax.fori_loop(0, R, reduce, zero))
        beta = rn / rr

        @pl.loop(0, R)
        def _(a):
            for j in range(3 * R):
                at = a * (3 * R) + j
                p1[at] = p1[at] + beta * p0[at]

        def third(a, carried):
            curve, total = carried[0], list(carried[1:])
            for b in range(R):
                stress, eps = stress_at(p1, a, b, None)
                for m in range(6):
                    total[m] = total[m] + stress[m]
                    curve = curve + stress[m] * eps[m]
                for i in range(3):
                    here = p1[i * CELLS + a * R + b]
                    curve = curve + (STAB * here) * here
            return (curve, *total)

        found = lax.fori_loop(0, R, third, (zero,) * 7)
        alpha1 = rn / across(found[0])
        for m in range(6):
            mean = jnp.sum(total0[m] + alpha0 * total1[m] + alpha1 * found[1 + m], axis=0, keepdims=True)
            av[pl.ds(case * 6 + m, 1), :] = mean * (1.0 / VOX)

        @pl.loop(0, CELLS)
        def _(cell):
            for i in range(3):
                at = i * CELLS + cell
                value = w[at] + alpha0 * p0[at] + alpha1 * p1[at]
                outb[pl.ds(case * CASE_ROWS + i * VOX + cell * R, R), :] = value[0:R, :]

        span = pl.ds(pl.multiple_of(case * CASE_ROWS, 8), CASE_ROWS)
        pltpu.make_async_copy(outb.at[span], new_ref.at[span], out_sem).start()
        return carry

    lax.fori_loop(0, CASES, case_body, 0)

    def send_rows(src, dst, rows, index):
        own = pl.ds(me * rows, rows)

        @pl.loop(1, NDEV)
        def _(k):
            d = lax.rem(me + k, NDEV)
            pltpu.make_async_remote_copy(
                src_ref=src.at[pl.ds(d * rows, rows)] if index == 5 else src,
                dst_ref=dst.at[own],
                send_sem=send_sem.at[index],
                recv_sem=recv_sem.at[index],
                device_id=dev(d),
                device_id_type=MESH,
            ).start()

    ret_out[...] = av[...].T
    send_rows(ret_out, ret_in, 1, 5)
    own_row = pl.ds(me, 1)
    own_copy = pltpu.make_async_copy(ret_out.at[own_row], ret_in.at[own_row], local_sem.at[5])
    own_copy.start()
    load_rows = zero
    for i in range(3):
        for y in range(2):
            dhalo[3, i : i + 1, 8 * y : 8 * y + 8] = load_ref[i, 0, y : y + 1, :]
    load_rows = jnp.where((lane < 16) & (row8 < 3), dhalo[3], 0.0)
    load_square = jnp.sum(load_rows * load_rows, keepdims=True)
    whole(ret_out, ret_in, 1, 5).wait_recv()
    own_copy.wait()
    back = ret_in[...].T
    home_rows = spread(home_dev)
    at_home = [lanes(back[8 * i : 8 * i + 8, :], home_rows) for i in range(6)]

    def averaged(case, m):
        row = case * 6 + m
        return at_home[row // 8][row % 8 : row % 8 + 1, :]

    grad = [float_ref[8 * k : 8 * k + 8, :] for k in range(3)]
    pick, mask = int_ref[0:8, :], float_ref[24:32, :]
    node_rows = []
    for kind in range(2):
        for i in range(3):
            value = zero
            for k, m in TERMS[i]:
                if kind == 0:
                    inner = spread(averaged(0, m))
                else:
                    inner = zero
                    for l, j in TERMS[i]:
                        inner = inner + grad[l] * averaged(1 + j, m)
                value = value + grad[k] * inner
            for step in (1, 2, 4):
                value = value + pltpu.roll(value, NDEV - step, axis=1)
            value = lanes(value, pick) * (mask * 0.125)
            node_rows.append(jnp.sum(value, axis=0, keepdims=True))
    tile = zero
    for r, value in enumerate(node_rows):
        tile = jnp.where(row8 == r, spread(value), tile)
    ntile[...] = tile
    part = load_rows - jnp.where(row8 < 3, tile, 0.0)
    first_row = part[0:1] + pltpu.roll(part[1:2], 64, axis=1)
    second_row = jnp.where(lane[0:1] == NDEV - 1, jnp.broadcast_to(load_square, (1, NDEV)), part[2:3])
    nrow[...] = jnp.concatenate([first_row, second_row], axis=0)
    nall[pl.ds(me * 2, 2), :] = jnp.concatenate([first_row, second_row], axis=0)
    halo_out = [near(3 + i, ntile, nhalo.at[i], s, r) for i, (s, r) in enumerate(steps)]
    for copy in halo_out:
        copy.start()
    send_rows(nrow, nall, 2, 6)

    for copy in halo_out:
        copy.wait()
    above = jnp.where(sub > 0, 1.0, 0.0).astype(F32)
    node = jnp.where(lane < 16, tile, 0.0)
    node = node + jnp.where(lane < 8, pltpu.roll(nhalo[0], NDEV - 16, axis=1), 0.0)
    node = node + jnp.where(lane < 16, pltpu.roll(nhalo[1], NDEV - 24, axis=1) * above, 0.0)
    node = node + jnp.where(lane < 8, pltpu.roll(nhalo[2], NDEV - 40, axis=1) * above, 0.0)
    residual = load_rows[0:3] - node[0:3]
    moved = dtile[0:3, :] + residual / jnp.maximum(node[3:6], FLOOR)
    for i in range(3):
        for y in range(2):
            displaced_ref[i, 0, y : y + 1, :] = moved[i : i + 1, 8 * y : 8 * y + 8]
            residual_ref[i, 0, y : y + 1, :] = residual[i : i + 1, 8 * y : 8 * y + 8]

    pltpu.make_async_remote_copy(
        src_ref=nall.at[pl.ds(0, 2 * NDEV - 2)],
        dst_ref=nall.at[pl.ds(0, 2 * NDEV - 2)],
        send_sem=send_sem.at[6],
        recv_sem=recv_sem.at[6],
        device_id=dev(lax.rem(me + 1, NDEV)),
        device_id_type=MESH,
    ).wait_recv()
    turn = jnp.where(lax.rem(row8, 4) == 0, row8 + 3, row8 - 1)
    square = zero
    load_sum = zero
    low = lax.rem(lane, 64)
    for half in range(2):
        before_z = zero
        for block in range(16):
            value = nall[pl.ds(block * 16 + half, 8, stride=2), :]
            if half == 1:
                load_sum = load_sum + jnp.where(lane == NDEV - 1, value, 0.0)
                value = jnp.where(lane < 64, value, 0.0)
            other = pltpu.roll(sublanes(value, turn), NDEV - 16, axis=1)
            value = value + jnp.where((low < 8) | ((low >= 24) & (low < 32)), other, 0.0)
            plane = pltpu.roll(value, NDEV - 24, axis=1)
            shifted = jnp.where(row8 < 4, pltpu.roll(before_z, 4, axis=0), pltpu.roll(plane, 4, axis=0))
            before_z = plane
            value = jnp.where(low < 16, value + shifted, 0.0)
            square = square + value * value
    norm_ref[...] = jnp.sqrt(jnp.sum(square, keepdims=True) / jnp.sum(load_sum, keepdims=True))

    for chunk in range(5):
        whole(sends[chunk], recvs[chunk], CHUNKS[chunk], chunk).wait_send()
    whole(ret_out, ret_in, 1, 5).wait_send()
    pltpu.make_async_remote_copy(
        src_ref=nall.at[pl.ds(0, 2 * NDEV - 2)],
        dst_ref=nall.at[pl.ds(0, 2 * NDEV - 2)],
        send_sem=send_sem.at[6],
        recv_sem=recv_sem.at[6],
        device_id=dev(lax.rem(me + 1, NDEV)),
        device_id_type=MESH,
    ).wait_send()
    pltpu.make_async_copy(outb, new_ref, out_sem).wait()


def per_device(displacement, load, home_slot, micro_state, state_slot, phases, phase_moduli):
    floats, ints = tables()
    vmem = pl.BlockSpec(memory_space=pltpu.VMEM)
    smem = pl.BlockSpec(memory_space=pltpu.SMEM)
    hbm = pl.BlockSpec(memory_space=pl.ANY)
    buffers = [pltpu.VMEM((NDEV * rows, NDEV), F32) for rows in CHUNKS]
    cells = pltpu.VMEM((3 * CELLS, 8, NDEV), F32)
    dma = pltpu.SemaphoreType.DMA
    new_state, displaced, residual, norm = pl.pallas_call(
        kernel,
        out_shape=(
            jax.ShapeDtypeStruct((ROWS, NDEV), F32),
            jax.ShapeDtypeStruct(displacement.shape, F32),
            jax.ShapeDtypeStruct(displacement.shape, F32),
            jax.ShapeDtypeStruct((1, 1), F32),
        ),
        in_specs=[vmem, vmem, vmem, vmem, smem, hbm, hbm, vmem, vmem],
        out_specs=(hbm, vmem, vmem, vmem),
        scratch_shapes=[
            pltpu.VMEM((ROWS + 72, NDEV), F32),
            pltpu.VMEM((VOX + 8, NDEV), jnp.int32),
            *buffers,
            *buffers,
            pltpu.VMEM((ROWS + 72, NDEV), F32),
            pltpu.VMEM((ROWS, NDEV), F32),
            pltpu.VMEM((CELLS, 8, NDEV), F32),
            pltpu.VMEM((CELLS, 8, NDEV), F32),
            cells,
            cells,
            cells,
            cells,
            pltpu.VMEM((6 * CELLS, 8, NDEV), F32),
            pltpu.VMEM((12, 8, NDEV), F32),
            pltpu.VMEM((NDEV, NDEV), F32),
            pltpu.VMEM((NDEV, NDEV), F32),
            pltpu.VMEM((NDEV, NDEV), F32),
            pltpu.VMEM((8, NDEV), F32),
            pltpu.VMEM((4, 8, NDEV), F32),
            pltpu.VMEM((8, NDEV), F32),
            pltpu.VMEM((3, 8, NDEV), F32),
            pltpu.VMEM((2, NDEV), F32),
            pltpu.VMEM((2 * NDEV, NDEV), F32),
            dma((CASES,)),
            dma,
            dma,
            dma((6,)),
            dma((7,)),
            dma((7,)),
            dma((6,)),
            dma((6,)),
        ],
        compiler_params=pltpu.CompilerParams(
            collective_id=1, has_side_effects=True, vmem_limit_bytes=48 * 1024 * 1024
        ),
    )(
        displacement,
        load,
        home_slot.reshape(1, NDEV),
        state_slot.reshape(1, NDEV),
        phase_moduli,
        micro_state.reshape(ROWS, NDEV),
        phases,
        jnp.asarray(floats),
        jnp.asarray(ints),
    )
    return new_state.reshape(CASES, 3, VOX, NDEV), displaced, residual, norm[0, 0]


def solution(mesh):
    both = ("sub", "rve")
    return jax.shard_map(
        per_device,
        mesh=mesh,
        in_specs=(
            P(None, "sub", "rve", None),
            P(None, "sub", "rve", None),
            P(both),
            P(None, None, None, both),
            P(both),
            P(None, both),
            P(),
        ),
        out_specs=(
            P(None, None, None, both),
            P(None, "sub", "rve", None),
            P(None, "sub", "rve", None),
            P(),
        ),
        check_vma=False,
    )
```

```python
import functools
import math

import jax
import jax.numpy as jnp
import numpy as np
from jax import lax
from jax.experimental import pallas as pl
from jax.experimental.pallas import tpu as pltpu
from jax.sharding import PartitionSpec as P

R = 6
VOX = 216
CASES = 7
STAB = 0.1
FLOOR = 1.0
NDEV = 128
NRVE = 4
NSUB = 32
ROWS = CASES * 3 * VOX
CASE_ROWS = 3 * VOX
CHUNKS = (6, 5, 5, 5, 5, 5, 5)
FIRST = (0, 6, 11, 16, 21, 26, 31)
LAST = len(CHUNKS) - 1
RETURN, NORM = LAST + 1, LAST + 2
CELLS = 36
LOGICAL = pl.DeviceIdType.LOGICAL
F32 = jnp.float32
TERMS = (((0, 0), (2, 4), (1, 5)), ((1, 1), (2, 3), (0, 5)), ((2, 2), (1, 3), (0, 4)))


def tables():
    offset = 0.5 / math.sqrt(3.0)
    places = (0.5 - offset, 0.5 + offset)
    slopes = np.zeros((3, 8, NDEV), np.float32)
    for g in range(NDEV):
        q = g % 8
        at = (places[q % 2], places[q // 2 % 2], places[q // 4])
        for a in range(8):
            bits = (a % 2, a // 2 % 2, a // 4)
            w = [at[k] if bits[k] else 1.0 - at[k] for k in range(3)]
            s = [1.0 if bits[k] else -1.0 for k in range(3)]
            slopes[0, a, g] = s[0] * w[1] * w[2]
            slopes[1, a, g] = w[0] * s[1] * w[2]
            slopes[2, a, g] = w[0] * w[1] * s[2]
    mask = np.zeros((8, NDEV), np.float32)
    pick = np.zeros((8, NDEV), np.int32)
    for n in range(48):
        nz, ny, nx = n // 24, n // 8 % 3, n % 8
        for a in range(8):
            ax, ay, az = a % 2, a // 2 % 2, a // 4
            ly = ny - ay
            if az == nz and 0 <= ly < 2:
                mask[a, n] = 1.0
                pick[a, n] = (ly * 8 + (nx - ax) % 8) * 8
    corner = np.zeros((8, NDEV), np.int32)
    for g in range(NDEV):
        ly, ex = g // 64, g // 8 % 8
        for a in range(8):
            ax, ay, az = a % 2, a // 2 % 2, a // 4
            corner[a, g] = az * 24 + (ly + ay) * 8 + (ex + ax) % 8
    floats = np.concatenate([slopes.reshape(24, NDEV), mask], axis=0)
    ints = np.concatenate([pick, corner], axis=0)
    return floats, ints


def around(step):
    return min(step, 4 - step)


SPREAD = [((i // 16 + i) % 4, (i // 4 + i) % 4, c, i % 4) for c in range(2) for i in range(64)][1:]
FARTHEST = sorted(SPREAD, key=lambda o: -(around(o[0]) + around(o[1]) + around(o[3]) + 0.3 * o[2]))


def lanes(x, index):
    return jnp.take_along_axis(x, index, axis=1, mode="promise_in_bounds")


def sublanes(x, index):
    return jnp.take_along_axis(x, index, axis=0, mode="promise_in_bounds")


def spread(row):
    return jnp.broadcast_to(row, (8, NDEV))


def inverse(target):
    column = jnp.broadcast_to(target, (NDEV, NDEV)).T
    lane = lax.broadcasted_iota(jnp.int32, (NDEV, NDEV), 1)
    row = lax.broadcasted_iota(jnp.int32, (NDEV, NDEV), 0)
    return jnp.sum(jnp.where(column == lane, row, 0).astype(F32), axis=0, keepdims=True).astype(jnp.int32)


def kernel(
    disp_hbm, load_hbm, home_hbm, state_hbm, moduli_hbm, float_hbm, int_hbm, micro_ref, phase_ref,
    new_ref, displaced_ref, residual_ref, norm_ref,
    disp_ref, load_ref, home_ref, state_slot_ref, moduli_ref, float_ref, int_ref, xin, ph, send0, send1, send2, send3, send4, send5, send6, recv0, recv1, recv2, recv3, recv4, recv5, recv6,
    nat, lam, mu, w, p0, p1, ap, sig, keep, av, ret_out, ret_in, dtile, dhalo, ntile, nhalo, nrow, nall,
    small_sem, in_sem, ph_sem, local_sem, send_sem, recv_sem, near_send, near_recv,
):
    sub, rve = lax.axis_index("sub"), lax.axis_index("rve")
    me = sub * NRVE + rve
    sends = (send0, send1, send2, send3, send4, send5, send6)
    recvs = (recv0, recv1, recv2, recv3, recv4, recv5, recv6)
    along_z = [lax.rem(sub // 8 + i, 4) * 32 for i in range(4)]
    along_y = [lax.rem(lax.rem(sub // 2, 4) + i, 4) * 8 for i in range(4)]
    along_c = [lax.rem(lax.rem(sub, 2) + i, 2) * 4 for i in range(2)]
    along_x = [lax.rem(rve + i, 4) for i in range(4)]

    def others(order):
        for z, y, c, x in order:
            yield along_z[z] + along_y[y] + (along_c[c] + along_x[x])

    other = along_z[0] + along_y[0] + (along_c[0] + along_x[1])

    barrier = pltpu.get_barrier_semaphore()

    for d in others(FARTHEST):
        pl.semaphore_signal(barrier, inc=1, device_id=d, device_id_type=LOGICAL)

    small = []
    pairs = (
        (state_hbm, state_slot_ref), (home_hbm, home_ref), (disp_hbm, disp_ref), (load_hbm, load_ref),
        (moduli_hbm, moduli_ref), (float_hbm, float_ref), (int_hbm, int_ref),
    )
    for i, (src, dst) in enumerate(pairs):
        small.append(pltpu.make_async_copy(src, dst, small_sem.at[i]))
        small[-1].start()

    loads = []
    for position in range(CASES):
        case = (position + 1) % CASES
        copy = pltpu.make_async_copy(
            micro_ref.at[pl.ds(case * CASE_ROWS, CASE_ROWS)],
            xin.at[pl.ds(position * CASE_ROWS, CASE_ROWS)],
            in_sem.at[position],
        )
        copy.start()
        loads.append(copy)
    phase_load = pltpu.make_async_copy(phase_ref, ph.at[pl.ds(0, VOX)], ph_sem)
    phase_load.start()

    for copy in small:
        copy.wait()
    dtile[...] = jnp.zeros((8, NDEV), F32)
    for i in range(3):
        for y in range(2):
            dtile[i : i + 1, 8 * y : 8 * y + 8] = disp_ref[i, 0, y : y + 1, :]

    home_dev = lax.shift_right_logical(home_ref[...], 7)
    state_index = spread(inverse(lax.shift_right_logical(state_slot_ref[...], 7)))
    home_index = spread(inverse(home_dev))

    def prepare(chunk, row, last):
        base = pl.multiple_of((FIRST[chunk] + row) * NDEV, NDEV)
        parts = []
        for i in range(16):
            if last and i > 7:
                parts.append(jnp.zeros((8, NDEV), F32))
            else:
                block = xin[pl.ds(base + 8 * i, 8), :]
                parts.append(lanes(block, home_index if last and i == 7 else state_index))
        pitch = CHUNKS[chunk]
        sends[chunk][pl.ds(row, NDEV, stride=pitch), :] = jnp.concatenate(parts, axis=0).T

    def prepare_chunk(chunk):
        for row in range(CHUNKS[chunk]):
            prepare(chunk, row, FIRST[chunk] + row == 35)

    def send_chunk(chunk):
        rows = CHUNKS[chunk]
        own = pl.ds(me * rows, rows)
        for d in others(SPREAD):
            pltpu.make_async_remote_copy(
                src_ref=sends[chunk].at[pl.ds(d * rows, rows)],
                dst_ref=recvs[chunk].at[own],
                send_sem=send_sem.at[chunk],
                recv_sem=recv_sem.at[chunk],
                device_id=d,
                device_id_type=LOGICAL,
            ).start()
        pltpu.make_async_copy(sends[chunk].at[own], recvs[chunk].at[own], local_sem.at[chunk]).start()

    def whole(src, dst, rows, index):
        return pltpu.make_async_remote_copy(
            src_ref=src.at[pl.ds(0, (NDEV - 1) * rows)],
            dst_ref=dst.at[pl.ds(0, (NDEV - 1) * rows)],
            send_sem=send_sem.at[index],
            recv_sem=recv_sem.at[index],
            device_id=other,
            device_id_type=LOGICAL,
        )

    for position in (0, 1):
        loads[position].wait()
    prepare_chunk(0)

    pl.semaphore_wait(barrier, NDEV - 1)

    def near(index, src, dst, dsub, drve):
        to_sub = lax.rem(sub + dsub + NSUB, NSUB)
        to_rve = lax.rem(rve + drve + NRVE, NRVE)
        return pltpu.make_async_remote_copy(
            src_ref=src,
            dst_ref=dst,
            send_sem=near_send.at[index],
            recv_sem=near_recv.at[index],
            device_id=to_sub * NRVE + to_rve,
            device_id_type=LOGICAL,
        )

    steps = ((0, 1), (1, 0), (1, 1))
    halo_in = [near(i, dtile, dhalo.at[i], -s, -r) for i, (s, r) in enumerate(steps)]
    for copy in halo_in:
        copy.start()
    send_chunk(0)
    for chunk in range(1, LAST):
        if chunk + 1 < CASES:
            loads[chunk + 1].wait()
        prepare_chunk(chunk)
        send_chunk(chunk)

    for copy in halo_in:
        copy.wait()
    lane = lax.broadcasted_iota(jnp.int32, (8, NDEV), 1)
    row8 = lax.broadcasted_iota(jnp.int32, (8, NDEV), 0)
    below = jnp.where(sub < NSUB - 1, 1.0, 0.0).astype(F32)
    extended = dtile[...]
    extended = jnp.where((lane >= 16) & (lane < 24), pltpu.roll(dhalo[0], 16, axis=1), extended)
    extended = jnp.where((lane >= 24) & (lane < 40), pltpu.roll(dhalo[1], 24, axis=1) * below, extended)
    extended = jnp.where((lane >= 40) & (lane < 48), pltpu.roll(dhalo[2], 40, axis=1) * below, extended)
    slope = [jnp.zeros((8, NDEV), F32) for _ in range(3)]
    for a in range(8):
        value = lanes(extended, spread(int_ref[8 + a : 9 + a, :]))
        for k in range(3):
            slope[k] = slope[k] + float_ref[8 * k + a : 8 * k + a + 1, :] * value
    s0, s1, s2 = slope
    strains = [
        s0[0:1], s1[1:2], s2[2:3],
        s2[1:2] + s1[2:3], s2[0:1] + s0[2:3], s1[0:1] + s0[1:2],
    ]
    strain_rows = jnp.zeros((8, NDEV), F32)
    for m in range(6):
        strain_rows = jnp.where(row8 == m, spread(strains[m]), strain_rows)
    xin[pl.ds(ROWS, 8), :] = strain_rows
    prepare_chunk(LAST)
    send_chunk(LAST)

    phase_load.wait()
    ph[pl.ds(VOX, 8), :] = jnp.zeros((8, NDEV), jnp.int32)
    inside = row8 < R
    moduli = [
        [jnp.broadcast_to(moduli_ref[which : which + 1, p : p + 1], (8, NDEV)) for p in range(3)] for which in range(2)
    ]

    @pl.loop(0, CELLS)
    def _(cell):
        label = ph[pl.ds(cell * R, 8), :]
        for which, out in ((0, lam), (1, mu)):
            value = jnp.where(
                label == 0,
                moduli[which][0],
                jnp.where(label == 1, moduli[which][1], moduli[which][2]),
            )
            out[cell] = jnp.where(inside, value, 0.0)

    av[...] = jnp.zeros((NDEV, NDEV), F32)
    up = jnp.where(row8 < 5, row8 + 1, jnp.where(row8 == 5, 0, row8))
    down = jnp.where(row8 == 0, 5, jnp.where(row8 < 6, row8 - 1, row8))

    def receive(chunk):
        rows = CHUNKS[chunk]
        own = pl.ds(me * rows, rows)
        whole(sends[chunk], recvs[chunk], rows, chunk).wait_recv()
        pltpu.make_async_copy(sends[chunk].at[own], recvs[chunk].at[own], local_sem.at[chunk]).wait()
        for row in range(rows):
            block = recvs[chunk][pl.ds(row, NDEV, stride=rows), :]
            nat[pl.ds((FIRST[chunk] + row) * NDEV, NDEV), :] = block.T

    zero = jnp.zeros((8, NDEV), F32)

    def stress_at(src, a, b, applied):
        following = lax.rem(a + 1, R)
        g = []
        for i in range(3):
            here = src[i * CELLS + a * R + b]
            g.append(
                (
                    src[i * CELLS + following * R + b] - here,
                    src[i * CELLS + a * R + (b + 1) % R] - here,
                    sublanes(here, up) - here,
                )
            )
        eps = [g[0][0], g[1][1], g[2][2], g[1][2] + g[2][1], g[0][2] + g[2][0], g[0][1] + g[1][0]]
        if applied is not None:
            eps = [eps[m] + applied[m] for m in range(6)]
        cell = a * R + b
        first, second = lam[cell], mu[cell]
        volume = first * (eps[0] + eps[1] + eps[2])
        twice = second + second
        stress = [volume + twice * eps[m] for m in range(3)] + [second * eps[m] for m in range(3, 6)]
        return stress, eps

    def stresses(src, applied):
        def body(a, total):
            total = list(total)
            for b in range(R):
                stress, _ = stress_at(src, a, b, applied)
                for m in range(6):
                    sig[m * CELLS + a * R + b] = stress[m]
                    total[m] = total[m] + stress[m]
            return tuple(total)

        return lax.fori_loop(0, R, body, (zero,) * 6)

    voigt = ((0, 5, 4), (5, 1, 3), (4, 3, 2))

    def force_at(src, a, b):
        before = lax.rem(a + R - 1, R)
        cell = a * R + b
        here = [sig[m * CELLS + cell] for m in range(6)]
        out = []
        for i in range(3):
            total = sig[voigt[0][i] * CELLS + before * R + b] - here[voigt[0][i]]
            total = total + (sig[voigt[1][i] * CELLS + a * R + (b + R - 1) % R] - here[voigt[1][i]])
            last = here[voigt[2][i]]
            total = total + (sublanes(last, down) - last)
            out.append(total + STAB * src[i * CELLS + cell])
        return out

    def across(x):
        return spread(jnp.sum(x, axis=0, keepdims=True))

    def finish(case):
        alpha0, alpha1 = keep[0], keep[1]

        @pl.loop(0, R)
        def _(a):
            for i in range(3):
                to = case * CASE_ROWS + i * VOX + a * (R * R)
                for b in range(R):
                    at = i * CELLS + a * R + b
                    value = w[at] + alpha0 * p0[at] + alpha1 * p1[at]
                    new_ref[pl.ds(to + b * R, R), :] = value[0:R, :]

    def case_body(position, carry):
        for chunk in range(CASES):

            @pl.when(position == chunk)
            def _():
                receive(chunk)

        case = lax.rem(position + 1, CASES)
        macro = nat[pl.ds(ROWS, 8), :]
        applied = []
        for m in range(6):
            unit = jnp.where(position == m, 1.0, 0.0).astype(F32)
            applied.append(jnp.where(position == CASES - 1, spread(macro[m : m + 1, :]), unit))

        @pl.loop(0, R)
        def _(a):
            for i in range(3):
                at = position * CASE_ROWS + i * VOX + a * (R * R)
                for b in range(R):
                    w[i * CELLS + a * R + b] = jnp.where(inside, nat[pl.ds(at + b * R, 8), :], 0.0)

        total0 = stresses(w, applied)

        def first(a, rr):
            for b in range(R):
                force = force_at(w, a, b)
                for i in range(3):
                    value = -force[i]
                    p0[i * CELLS + a * R + b] = value
                    force[i] = value * value
                rr = rr + (force[0] + (force[1] + force[2]))
            return rr

        rr = across(lax.fori_loop(0, R, first, zero))
        total1 = stresses(p0, None)

        def second(a, curve):
            for b in range(R):
                force = force_at(p0, a, b)
                for i in range(3):
                    ap[i * CELLS + a * R + b] = force[i]
                    force[i] = p0[i * CELLS + a * R + b] * force[i]
                curve = curve + (force[0] + (force[1] + force[2]))
            return curve

        alpha0 = rr / across(lax.fori_loop(0, R, second, zero))

        def reduce(a, total):
            total = list(total)
            for j in range(3 * R):
                at = a * (3 * R) + j
                value = p0[at] - alpha0 * ap[at]
                p1[at] = value
                total[j % 6] = total[j % 6] + value * value
            return tuple(total)

        parts = lax.fori_loop(0, R, reduce, (zero,) * 6)
        rn = across(((parts[0] + parts[1]) + (parts[2] + parts[3])) + (parts[4] + parts[5]))
        beta = rn / rr

        @pl.loop(0, R)
        def _(a):
            for j in range(3 * R):
                at = a * (3 * R) + j
                p1[at] = p1[at] + beta * p0[at]

        def third(a, carried):
            curve, total = carried[0], list(carried[1:])
            for b in range(R):
                stress, eps = stress_at(p1, a, b, None)
                for m in range(6):
                    total[m] = total[m] + stress[m]
                work = [stress[m] * eps[m] for m in range(6)]
                here = [p1[i * CELLS + a * R + b] for i in range(3)]
                kept = STAB * ((here[0] * here[0] + here[1] * here[1]) + here[2] * here[2])
                curve = curve + (((work[0] + work[1]) + (work[2] + work[3])) + ((work[4] + work[5]) + kept))
            return (curve, *total)

        found = lax.fori_loop(0, R, third, (zero,) * 7)
        alpha1 = rn / across(found[0])
        for m in range(6):
            mean = jnp.sum(total0[m] + alpha0 * total1[m] + alpha1 * found[1 + m], axis=0, keepdims=True)
            av[pl.ds(case * 6 + m, 1), :] = mean * (1.0 / VOX)

        keep[0], keep[1] = alpha0, alpha1

        @pl.when(position < LAST)
        def _():
            finish(case)

        return carry

    lax.fori_loop(0, CASES, case_body, 0)

    def send_rows(src, dst, rows, index):
        own = pl.ds(me * rows, rows)
        for d in others(FARTHEST):
            pltpu.make_async_remote_copy(
                src_ref=src.at[pl.ds(d, 1)] if index == RETURN else src,
                dst_ref=dst.at[own],
                send_sem=send_sem.at[index],
                recv_sem=recv_sem.at[index],
                device_id=d,
                device_id_type=LOGICAL,
            ).start()

    ret_out[...] = av[...].T
    send_rows(ret_out, ret_in, 1, RETURN)
    own_row = pl.ds(me, 1)
    own_copy = pltpu.make_async_copy(ret_out.at[own_row], ret_in.at[own_row], local_sem.at[RETURN])
    own_copy.start()
    finish(0)
    for i in range(3):
        for y in range(2):
            dhalo[3, i : i + 1, 8 * y : 8 * y + 8] = load_ref[i, 0, y : y + 1, :]
    load_rows = jnp.where((lane < 16) & (row8 < 3), dhalo[3], 0.0)
    load_square = jnp.sum(load_rows * load_rows, keepdims=True)
    whole(ret_out, ret_in, 1, RETURN).wait_recv()
    own_copy.wait()
    back = ret_in[...].T
    home_rows = spread(home_dev)
    at_home = [lanes(back[8 * i : 8 * i + 8, :], home_rows) for i in range(6)]

    def averaged(case, m):
        row = case * 6 + m
        return at_home[row // 8][row % 8 : row % 8 + 1, :]

    grad = [float_ref[8 * k : 8 * k + 8, :] for k in range(3)]
    pick, mask = int_ref[0:8, :], float_ref[24:32, :]
    node_rows = []
    for kind in range(2):
        for i in range(3):
            value = zero
            for k, m in TERMS[i]:
                if kind == 0:
                    inner = spread(averaged(0, m))
                else:
                    inner = zero
                    for l, j in TERMS[i]:
                        inner = inner + grad[l] * averaged(1 + j, m)
                value = value + grad[k] * inner
            for step in (1, 2, 4):
                value = value + pltpu.roll(value, NDEV - step, axis=1)
            value = lanes(value, pick) * (mask * 0.125)
            node_rows.append(jnp.sum(value, axis=0, keepdims=True))
    tile = zero
    for r, value in enumerate(node_rows):
        tile = jnp.where(row8 == r, spread(value), tile)
    ntile[...] = tile
    part = load_rows - jnp.where(row8 < 3, tile, 0.0)
    first_row = part[0:1] + pltpu.roll(part[1:2], 64, axis=1)
    second_row = jnp.where(lane[0:1] == NDEV - 1, jnp.broadcast_to(load_square, (1, NDEV)), part[2:3])
    nrow[...] = jnp.concatenate([first_row, second_row], axis=0)
    nall[pl.ds(me * 2, 2), :] = jnp.concatenate([first_row, second_row], axis=0)
    halo_out = [near(3 + i, ntile, nhalo.at[i], s, r) for i, (s, r) in enumerate(steps)]
    for copy in halo_out:
        copy.start()
    send_rows(nrow, nall, 2, NORM)

    for copy in halo_out:
        copy.wait()
    above = jnp.where(sub > 0, 1.0, 0.0).astype(F32)
    node = jnp.where(lane < 16, tile, 0.0)
    node = node + jnp.where(lane < 8, pltpu.roll(nhalo[0], NDEV - 16, axis=1), 0.0)
    node = node + jnp.where(lane < 16, pltpu.roll(nhalo[1], NDEV - 24, axis=1) * above, 0.0)
    node = node + jnp.where(lane < 8, pltpu.roll(nhalo[2], NDEV - 40, axis=1) * above, 0.0)
    residual = load_rows[0:3] - node[0:3]
    moved = dtile[0:3, :] + residual / jnp.maximum(node[3:6], FLOOR)
    for i in range(3):
        for y in range(2):
            displaced_ref[i, 0, y : y + 1, :] = moved[i : i + 1, 8 * y : 8 * y + 8]
            residual_ref[i, 0, y : y + 1, :] = residual[i : i + 1, 8 * y : 8 * y + 8]

    pltpu.make_async_remote_copy(
        src_ref=nall.at[pl.ds(0, 2 * NDEV - 2)],
        dst_ref=nall.at[pl.ds(0, 2 * NDEV - 2)],
        send_sem=send_sem.at[NORM],
        recv_sem=recv_sem.at[NORM],
        device_id=other,
        device_id_type=LOGICAL,
    ).wait_recv()
    turn = jnp.where(lax.rem(row8, 4) == 0, row8 + 3, row8 - 1)
    square = zero
    load_sum = zero
    low = lax.rem(lane, 64)
    for half in range(2):
        before_z = zero
        for block in range(16):
            value = nall[pl.ds(block * 16 + half, 8, stride=2), :]
            if half == 1:
                load_sum = load_sum + jnp.where(lane == NDEV - 1, value, 0.0)
                value = jnp.where(lane < 64, value, 0.0)
            other = pltpu.roll(sublanes(value, turn), NDEV - 16, axis=1)
            value = value + jnp.where((low < 8) | ((low >= 24) & (low < 32)), other, 0.0)
            plane = pltpu.roll(value, NDEV - 24, axis=1)
            shifted = jnp.where(row8 < 4, pltpu.roll(before_z, 4, axis=0), pltpu.roll(plane, 4, axis=0))
            before_z = plane
            value = jnp.where(low < 16, value + shifted, 0.0)
            square = square + value * value
    norm_ref[...] = jnp.sqrt(jnp.sum(square, keepdims=True) / jnp.sum(load_sum, keepdims=True))

    for chunk in range(CASES):
        whole(sends[chunk], recvs[chunk], CHUNKS[chunk], chunk).wait_send()
    whole(ret_out, ret_in, 1, RETURN).wait_send()
    pltpu.make_async_remote_copy(
        src_ref=nall.at[pl.ds(0, 2 * NDEV - 2)],
        dst_ref=nall.at[pl.ds(0, 2 * NDEV - 2)],
        send_sem=send_sem.at[NORM],
        recv_sem=recv_sem.at[NORM],
        device_id=other,
        device_id_type=LOGICAL,
    ).wait_send()


def per_device(displacement, load, home_slot, micro_state, state_slot, phases, phase_moduli):
    floats, ints = tables()
    vmem = pl.BlockSpec(memory_space=pltpu.VMEM)
    hbm = pl.BlockSpec(memory_space=pltpu.HBM)
    buffers = [pltpu.VMEM((NDEV * rows, NDEV), F32) for rows in CHUNKS]
    cells = pltpu.VMEM((3 * CELLS, 8, NDEV), F32)
    dma = pltpu.SemaphoreType.DMA
    arguments = (
        displacement,
        load,
        home_slot.reshape(1, NDEV),
        state_slot.reshape(1, NDEV),
        phase_moduli,
        jnp.asarray(floats),
        jnp.asarray(ints),
        micro_state.reshape(ROWS, NDEV),
        phases,
    )
    new_state, displaced, residual, norm = pl.pallas_call(
        kernel,
        out_shape=(
            pltpu.VMEM((ROWS, NDEV), F32),
            pltpu.VMEM(displacement.shape, F32),
            pltpu.VMEM(displacement.shape, F32),
            jax.ShapeDtypeStruct((1, 1), F32),
        ),
        in_specs=[hbm] * 9,
        out_specs=(vmem,) * 4,
        scratch_shapes=[
            pltpu.VMEM(displacement.shape, F32),
            pltpu.VMEM(load.shape, F32),
            pltpu.VMEM((1, NDEV), jnp.int32),
            pltpu.VMEM((1, NDEV), jnp.int32),
            pltpu.VMEM(phase_moduli.shape, F32),
            pltpu.VMEM(floats.shape, F32),
            pltpu.VMEM(ints.shape, jnp.int32),
            pltpu.VMEM((ROWS + 72, NDEV), F32),
            pltpu.VMEM((VOX + 8, NDEV), jnp.int32),
            *buffers,
            *buffers,
            pltpu.VMEM((ROWS + 72, NDEV), F32),
            pltpu.VMEM((CELLS, 8, NDEV), F32),
            pltpu.VMEM((CELLS, 8, NDEV), F32),
            cells,
            cells,
            cells,
            cells,
            pltpu.VMEM((6 * CELLS, 8, NDEV), F32),
            pltpu.VMEM((2, 8, NDEV), F32),
            pltpu.VMEM((NDEV, NDEV), F32),
            pltpu.VMEM((NDEV, NDEV), F32),
            pltpu.VMEM((NDEV, NDEV), F32),
            pltpu.VMEM((8, NDEV), F32),
            pltpu.VMEM((4, 8, NDEV), F32),
            pltpu.VMEM((8, NDEV), F32),
            pltpu.VMEM((3, 8, NDEV), F32),
            pltpu.VMEM((2, NDEV), F32),
            pltpu.VMEM((2 * NDEV, NDEV), F32),
            dma((7,)),
            dma((CASES,)),
            dma,
            dma((CASES + 1,)),
            dma((CASES + 2,)),
            dma((CASES + 2,)),
            dma((6,)),
            dma((6,)),
        ],
        compiler_params=pltpu.CompilerParams(
            collective_id=1, has_side_effects=True, vmem_limit_bytes=48 * 1024 * 1024
        ),
    )(*[pltpu.with_memory_space_constraint(x, pltpu.HBM) for x in arguments])
    return new_state.reshape(CASES, 3, VOX, NDEV), displaced, residual, norm[0, 0]


def solution(mesh):
    both = ("sub", "rve")
    return jax.shard_map(
        per_device,
        mesh=mesh,
        in_specs=(
            P(None, "sub", "rve", None),
            P(None, "sub", "rve", None),
            P(both),
            P(None, None, None, both),
            P(both),
            P(None, both),
            P(),
        ),
        out_specs=(
            P(None, None, None, both),
            P(None, "sub", "rve", None),
            P(None, "sub", "rve", None),
            P(),
        ),
        check_vma=False,
    )
```

```python
import functools
import math

import jax
import jax.numpy as jnp
import numpy as np
from jax import lax
from jax.experimental import pallas as pl
from jax.experimental.pallas import tpu as pltpu
from jax.sharding import PartitionSpec as P

R = 6
VOX = 216
CASES = 7
STAB = 0.1
FLOOR = 1.0
NDEV = 128
NRVE = 4
NSUB = 32
ROWS = CASES * 3 * VOX
CASE_ROWS = 3 * VOX
CHUNKS = (6, 5, 5, 5, 5, 5, 5)
FIRST = (0, 6, 11, 16, 21, 26, 31)
LAST = len(CHUNKS) - 1
ORDER = (1, 2, 0, 3, 4, 5, 6)
MACRO = 2
STRAIN_ROW = 3 * CASE_ROWS
STRESS_ROW = 7 * CASE_ROWS + 8
RETURN, NORM = LAST + 1, LAST + 2
CELLS = 36
LOGICAL = pl.DeviceIdType.LOGICAL
F32 = jnp.float32
TERMS = (((0, 0), (2, 4), (1, 5)), ((1, 1), (2, 3), (0, 5)), ((2, 2), (1, 3), (0, 4)))


def tables():
    offset = 0.5 / math.sqrt(3.0)
    places = (0.5 - offset, 0.5 + offset)
    slopes = np.zeros((3, 8, NDEV), np.float32)
    for g in range(NDEV):
        q = g % 8
        at = (places[q % 2], places[q // 2 % 2], places[q // 4])
        for a in range(8):
            bits = (a % 2, a // 2 % 2, a // 4)
            w = [at[k] if bits[k] else 1.0 - at[k] for k in range(3)]
            s = [1.0 if bits[k] else -1.0 for k in range(3)]
            slopes[0, a, g] = s[0] * w[1] * w[2]
            slopes[1, a, g] = w[0] * s[1] * w[2]
            slopes[2, a, g] = w[0] * w[1] * s[2]
    mask = np.zeros((8, NDEV), np.float32)
    pick = np.zeros((8, NDEV), np.int32)
    for n in range(48):
        nz, ny, nx = n // 24, n // 8 % 3, n % 8
        for a in range(8):
            ax, ay, az = a % 2, a // 2 % 2, a // 4
            ly = ny - ay
            if az == nz and 0 <= ly < 2:
                mask[a, n] = 1.0
                pick[a, n] = (ly * 8 + (nx - ax) % 8) * 8
    corner = np.zeros((8, NDEV), np.int32)
    for g in range(NDEV):
        ly, ex = g // 64, g // 8 % 8
        for a in range(8):
            ax, ay, az = a % 2, a // 2 % 2, a // 4
            corner[a, g] = az * 24 + (ly + ay) * 8 + (ex + ax) % 8
    floats = np.concatenate([slopes.reshape(24, NDEV), mask], axis=0)
    ints = np.concatenate([pick, corner], axis=0)
    return floats, ints


def base_of(position):
    return position * CASE_ROWS + 8 * ((position + 3) // 6)


def around(step):
    return min(step, 4 - step)


SPREAD = [((i // 16 + i) % 4, (i // 4 + i) % 4, c, i % 4) for c in range(2) for i in range(64)][1:]
FARTHEST = sorted(SPREAD, key=lambda o: -(around(o[0]) + around(o[1]) + around(o[3]) + 0.3 * o[2]))


def lanes(x, index):
    return jnp.take_along_axis(x, index, axis=1, mode="promise_in_bounds")


def sublanes(x, index):
    return jnp.take_along_axis(x, index, axis=0, mode="promise_in_bounds")


def spread(row):
    return jnp.broadcast_to(row, (8, NDEV))


def inverse(target):
    column = jnp.broadcast_to(target, (NDEV, NDEV)).T
    lane = lax.broadcasted_iota(jnp.int32, (NDEV, NDEV), 1)
    row = lax.broadcasted_iota(jnp.int32, (NDEV, NDEV), 0)
    return jnp.sum(jnp.where(column == lane, row, 0).astype(F32), axis=0, keepdims=True).astype(jnp.int32)


def kernel(
    disp_hbm, load_hbm, home_hbm, state_hbm, moduli_hbm, float_hbm, int_hbm, micro_ref, phase_ref,
    new_ref, displaced_ref, residual_ref, norm_ref,
    disp_ref, load_ref, home_ref, state_slot_ref, moduli_ref, float_ref, int_ref, xin, ph, send0, send1, send2, send3, send4, send5, send6, recv0, recv1, recv2, recv3, recv4, recv5, recv6,
    nat, lam, mu, w, p0, p1, ap, sig, keep, av, ret_out, ret_in, dtile, dhalo, ntile, nhalo, nrow, nall, whole_residual,
    small_sem, in_sem, ph_sem, local_sem, send_sem, recv_sem, near_send, near_recv,
):
    sub, rve = lax.axis_index("sub"), lax.axis_index("rve")
    me = sub * NRVE + rve
    sends = (send0, send1, send2, send3, send4, send5, send6)
    recvs = (recv0, recv1, recv2, recv3, recv4, recv5, recv6)
    along_z = [lax.rem(sub // 8 + i, 4) * 32 for i in range(4)]
    along_y = [lax.rem(lax.rem(sub // 2, 4) + i, 4) * 8 for i in range(4)]
    along_c = [lax.rem(lax.rem(sub, 2) + i, 2) * 4 for i in range(2)]
    along_x = [lax.rem(rve + i, 4) for i in range(4)]

    def others(order):
        for z, y, c, x in order:
            yield along_z[z] + along_y[y] + (along_c[c] + along_x[x])

    other = along_z[0] + along_y[0] + (along_c[0] + along_x[1])

    barrier = pltpu.get_barrier_semaphore()

    for d in others(FARTHEST):
        pl.semaphore_signal(barrier, inc=1, device_id=d, device_id_type=LOGICAL)

    small = []
    pairs = (
        (state_hbm, state_slot_ref), (home_hbm, home_ref), (disp_hbm, disp_ref), (load_hbm, load_ref),
        (moduli_hbm, moduli_ref), (float_hbm, float_ref), (int_hbm, int_ref),
    )
    for i, (src, dst) in enumerate(pairs):
        small.append(pltpu.make_async_copy(src, dst, small_sem.at[i]))
        small[-1].start()

    loads = []
    for position, case in enumerate(ORDER):
        copy = pltpu.make_async_copy(
            micro_ref.at[pl.ds(case * CASE_ROWS, CASE_ROWS)],
            xin.at[pl.ds(base_of(position), CASE_ROWS)],
            in_sem.at[position],
        )
        copy.start()
        loads.append(copy)
    phase_load = pltpu.make_async_copy(phase_ref, ph.at[pl.ds(0, VOX)], ph_sem)
    phase_load.start()

    for copy in small:
        copy.wait()
    dtile[...] = jnp.zeros((8, NDEV), F32)
    for i in range(3):
        for y in range(2):
            dtile[i : i + 1, 8 * y : 8 * y + 8] = disp_ref[i, 0, y : y + 1, :]

    home_dev = lax.shift_right_logical(home_ref[...], 7)
    state_index = spread(inverse(lax.shift_right_logical(state_slot_ref[...], 7)))
    home_index = spread(inverse(home_dev))

    def prepare(chunk, row):
        parts = []
        for i in range(16):
            at = (FIRST[chunk] + row) * NDEV + 8 * i
            block = xin[pl.ds(at, 8), :]
            if at == STRAIN_ROW:
                block = lanes(block, home_index)
            elif at != STRESS_ROW:
                block = lanes(block, state_index)
            parts.append(block)
        sends[chunk][pl.ds(row, NDEV, stride=CHUNKS[chunk]), :] = jnp.concatenate(parts, axis=0).T

    def prepare_chunk(chunk):
        for row in range(CHUNKS[chunk]):
            prepare(chunk, row)

    def send_chunk(chunk):
        rows = CHUNKS[chunk]
        own = pl.ds(me * rows, rows)
        for d in others(SPREAD):
            pltpu.make_async_remote_copy(
                src_ref=sends[chunk].at[pl.ds(d * rows, rows)],
                dst_ref=recvs[chunk].at[own],
                send_sem=send_sem.at[chunk],
                recv_sem=recv_sem.at[chunk],
                device_id=d,
                device_id_type=LOGICAL,
            ).start()
        pltpu.make_async_copy(sends[chunk].at[own], recvs[chunk].at[own], local_sem.at[chunk]).start()

    def whole(src, dst, rows, index):
        return pltpu.make_async_remote_copy(
            src_ref=src.at[pl.ds(0, (NDEV - 1) * rows)],
            dst_ref=dst.at[pl.ds(0, (NDEV - 1) * rows)],
            send_sem=send_sem.at[index],
            recv_sem=recv_sem.at[index],
            device_id=other,
            device_id_type=LOGICAL,
        )

    for position in (0, 1):
        loads[position].wait()
    prepare_chunk(0)

    pl.semaphore_wait(barrier, NDEV - 1)

    def near(index, src, dst, dsub, drve):
        to_sub = lax.rem(sub + dsub + NSUB, NSUB)
        to_rve = lax.rem(rve + drve + NRVE, NRVE)
        return pltpu.make_async_remote_copy(
            src_ref=src,
            dst_ref=dst,
            send_sem=near_send.at[index],
            recv_sem=near_recv.at[index],
            device_id=to_sub * NRVE + to_rve,
            device_id_type=LOGICAL,
        )

    steps = ((0, 1), (1, 0), (1, 1))
    halo_in = [near(i, dtile, dhalo.at[i], -s, -r) for i, (s, r) in enumerate(steps)]
    for copy in halo_in:
        copy.start()
    send_chunk(0)
    loads[2].wait()
    prepare_chunk(1)
    send_chunk(1)

    for copy in halo_in:
        copy.wait()
    lane = lax.broadcasted_iota(jnp.int32, (8, NDEV), 1)
    row8 = lax.broadcasted_iota(jnp.int32, (8, NDEV), 0)
    below = jnp.where(sub < NSUB - 1, 1.0, 0.0).astype(F32)
    extended = dtile[...]
    extended = jnp.where((lane >= 16) & (lane < 24), pltpu.roll(dhalo[0], 16, axis=1), extended)
    extended = jnp.where((lane >= 24) & (lane < 40), pltpu.roll(dhalo[1], 24, axis=1) * below, extended)
    extended = jnp.where((lane >= 40) & (lane < 48), pltpu.roll(dhalo[2], 40, axis=1) * below, extended)
    slope = [jnp.zeros((8, NDEV), F32) for _ in range(3)]
    for a in range(8):
        value = lanes(extended, spread(int_ref[8 + a : 9 + a, :]))
        for k in range(3):
            slope[k] = slope[k] + float_ref[8 * k + a : 8 * k + a + 1, :] * value
    s0, s1, s2 = slope
    strains = [
        s0[0:1], s1[1:2], s2[2:3],
        s2[1:2] + s1[2:3], s2[0:1] + s0[2:3], s1[0:1] + s0[1:2],
    ]
    strain_rows = jnp.zeros((8, NDEV), F32)
    for m in range(6):
        strain_rows = jnp.where(row8 == m, spread(strains[m]), strain_rows)
    xin[pl.ds(STRAIN_ROW, 8), :] = strain_rows
    for chunk in range(MACRO, LAST):
        loads[chunk + 1].wait()
        prepare_chunk(chunk)
        send_chunk(chunk)
    xin[pl.ds(STRESS_ROW + 8, 56), :] = jnp.zeros((56, NDEV), F32)

    phase_load.wait()
    ph[pl.ds(VOX, 8), :] = jnp.zeros((8, NDEV), jnp.int32)
    inside = row8 < R
    moduli = [
        [jnp.broadcast_to(moduli_ref[which : which + 1, p : p + 1], (8, NDEV)) for p in range(3)] for which in range(2)
    ]

    @pl.loop(0, CELLS)
    def _(cell):
        label = ph[pl.ds(cell * R, 8), :]
        for which, out in ((0, lam), (1, mu)):
            value = jnp.where(
                label == 0,
                moduli[which][0],
                jnp.where(label == 1, moduli[which][1], moduli[which][2]),
            )
            out[cell] = jnp.where(inside, value, 0.0)

    av[...] = jnp.zeros((NDEV, NDEV), F32)
    up = jnp.where(row8 < 5, row8 + 1, jnp.where(row8 == 5, 0, row8))
    down = jnp.where(row8 == 0, 5, jnp.where(row8 < 6, row8 - 1, row8))

    def receive(chunk):
        rows = CHUNKS[chunk]
        own = pl.ds(me * rows, rows)
        whole(sends[chunk], recvs[chunk], rows, chunk).wait_recv()
        pltpu.make_async_copy(sends[chunk].at[own], recvs[chunk].at[own], local_sem.at[chunk]).wait()
        for row in range(rows):
            block = recvs[chunk][pl.ds(row, NDEV, stride=rows), :]
            nat[pl.ds((FIRST[chunk] + row) * NDEV, NDEV), :] = block.T

    zero = jnp.zeros((8, NDEV), F32)

    def stress_at(src, a, b, applied):
        following = lax.rem(a + 1, R)
        g = []
        for i in range(3):
            here = src[i * CELLS + a * R + b]
            g.append(
                (
                    src[i * CELLS + following * R + b] - here,
                    src[i * CELLS + a * R + (b + 1) % R] - here,
                    sublanes(here, up) - here,
                )
            )
        eps = [g[0][0], g[1][1], g[2][2], g[1][2] + g[2][1], g[0][2] + g[2][0], g[0][1] + g[1][0]]
        if applied is not None:
            eps = [eps[m] + applied[m] for m in range(6)]
        cell = a * R + b
        first, second = lam[cell], mu[cell]
        volume = first * (eps[0] + eps[1] + eps[2])
        twice = second + second
        stress = [volume + twice * eps[m] for m in range(3)] + [second * eps[m] for m in range(3, 6)]
        return stress, eps

    def stresses(src, applied):
        def body(a, total):
            total = list(total)
            for b in range(R):
                stress, _ = stress_at(src, a, b, applied)
                for m in range(6):
                    sig[m * CELLS + a * R + b] = stress[m]
                    total[m] = total[m] + stress[m]
            return tuple(total)

        return lax.fori_loop(0, R, body, (zero,) * 6)

    voigt = ((0, 5, 4), (5, 1, 3), (4, 3, 2))

    def force_at(src, a, b):
        before = lax.rem(a + R - 1, R)
        cell = a * R + b
        here = [sig[m * CELLS + cell] for m in range(6)]
        out = []
        for i in range(3):
            total = sig[voigt[0][i] * CELLS + before * R + b] - here[voigt[0][i]]
            total = total + (sig[voigt[1][i] * CELLS + a * R + (b + R - 1) % R] - here[voigt[1][i]])
            last = here[voigt[2][i]]
            total = total + (sublanes(last, down) - last)
            out.append(total + STAB * src[i * CELLS + cell])
        return out

    def across(x):
        return spread(jnp.sum(x, axis=0, keepdims=True))

    def finish(case):
        alpha0, alpha1 = keep[0], keep[1]

        @pl.loop(0, R)
        def _(a):
            for i in range(3):
                to = case * CASE_ROWS + i * VOX + a * (R * R)
                for b in range(R):
                    at = i * CELLS + a * R + b
                    value = w[at] + alpha0 * p0[at] + alpha1 * p1[at]
                    new_ref[pl.ds(to + b * R, R), :] = value[0:R, :]

    for i in range(3):
        for y in range(2):
            dhalo[3, i : i + 1, 8 * y : 8 * y + 8] = load_ref[i, 0, y : y + 1, :]
    home_rows = spread(home_dev)
    grad = [float_ref[8 * k : 8 * k + 8, :] for k in range(3)]

    def to_nodes(value):
        for step in (1, 2, 4):
            value = value + pltpu.roll(value, NDEV - step, axis=1)
        value = lanes(value, int_ref[0:8, :]) * (float_ref[24:32, :] * 0.125)
        return jnp.sum(value, axis=0, keepdims=True)

    def tiled(rows):
        tile = zero
        for r, value in enumerate(rows):
            tile = jnp.where(row8 == r, spread(value), tile)
        return tile

    def assemble_force():
        stress = lanes(nat[pl.ds(STRESS_ROW, 8), :], home_rows)
        rows = []
        for i in range(3):
            value = zero
            for k, m in TERMS[i]:
                value = value + grad[k] * spread(stress[m : m + 1, :])
            rows.append(to_nodes(value))
        load_rows = jnp.where((lane < 16) & (row8 < 3), dhalo[3], 0.0)
        load_square = jnp.sum(load_rows * load_rows, keepdims=True)
        part = load_rows - tiled(rows)
        first_row = part[0:1] + pltpu.roll(part[1:2], 64, axis=1)
        second_row = jnp.where(lane[0:1] == NDEV - 1, jnp.broadcast_to(load_square, (1, NDEV)), part[2:3])
        both = jnp.concatenate([first_row, second_row], axis=0)
        nrow[...] = both
        nall[pl.ds(me * 2, 2), :] = both

    def case_body(position, carry):
        for chunk in range(CASES):

            @pl.when(position == chunk)
            def _():
                receive(chunk)

        plain = (position + 3) // 6
        case = plain * position + (1 - plain) * lax.rem(position + 1, 3)
        macro = nat[pl.ds(STRAIN_ROW, 8), :]
        applied = []
        for m in range(6):
            unit = jnp.where(case == m + 1, 1.0, 0.0).astype(F32)
            applied.append(jnp.where(position == MACRO, spread(macro[m : m + 1, :]), unit))

        @pl.loop(0, R)
        def _(a):
            for i in range(3):
                at = base_of(position) + i * VOX + a * (R * R)
                for b in range(R):
                    w[i * CELLS + a * R + b] = jnp.where(inside, nat[pl.ds(at + b * R, 8), :], 0.0)

        total0 = stresses(w, applied)

        def first(a, rr):
            for b in range(R):
                force = force_at(w, a, b)
                for i in range(3):
                    value = -force[i]
                    p0[i * CELLS + a * R + b] = value
                    force[i] = value * value
                rr = rr + (force[0] + (force[1] + force[2]))
            return rr

        rr = across(lax.fori_loop(0, R, first, zero))
        total1 = stresses(p0, None)

        def second(a, curve):
            for b in range(R):
                force = force_at(p0, a, b)
                for i in range(3):
                    ap[i * CELLS + a * R + b] = force[i]
                    force[i] = p0[i * CELLS + a * R + b] * force[i]
                curve = curve + (force[0] + (force[1] + force[2]))
            return curve

        alpha0 = rr / across(lax.fori_loop(0, R, second, zero))

        def reduce(a, total):
            total = list(total)
            for j in range(3 * R):
                at = a * (3 * R) + j
                value = p0[at] - alpha0 * ap[at]
                p1[at] = value
                total[j % 6] = total[j % 6] + value * value
            return tuple(total)

        parts = lax.fori_loop(0, R, reduce, (zero,) * 6)
        rn = across(((parts[0] + parts[1]) + (parts[2] + parts[3])) + (parts[4] + parts[5]))
        beta = rn / rr

        @pl.loop(0, R)
        def _(a):
            for j in range(3 * R):
                at = a * (3 * R) + j
                p1[at] = p1[at] + beta * p0[at]

        def third(a, carried):
            curve, total = carried[0], list(carried[1:])
            for b in range(R):
                stress, eps = stress_at(p1, a, b, None)
                for m in range(6):
                    total[m] = total[m] + stress[m]
                work = [stress[m] * eps[m] for m in range(6)]
                here = [p1[i * CELLS + a * R + b] for i in range(3)]
                kept = STAB * ((here[0] * here[0] + here[1] * here[1]) + here[2] * here[2])
                curve = curve + (((work[0] + work[1]) + (work[2] + work[3])) + ((work[4] + work[5]) + kept))
            return (curve, *total)

        found = lax.fori_loop(0, R, third, (zero,) * 7)
        alpha1 = rn / across(found[0])
        for m in range(6):
            mean = jnp.sum(total0[m] + alpha0 * total1[m] + alpha1 * found[1 + m], axis=0, keepdims=True)
            av[pl.ds(case * 6 + m, 1), :] = mean * (1.0 / VOX)

        keep[0], keep[1] = alpha0, alpha1

        @pl.when(position < LAST)
        def _():
            finish(case)

        @pl.when(position == MACRO)
        def _():
            xin[pl.ds(STRESS_ROW, 8), :] = av[0:8, :]
            prepare_chunk(LAST)
            send_chunk(LAST)

        return carry

    lax.fori_loop(0, CASES, case_body, 0)

    def send_rows(src, dst, rows, index):
        own = pl.ds(me * rows, rows)
        for d in others(FARTHEST):
            pltpu.make_async_remote_copy(
                src_ref=src.at[pl.ds(d, 1)] if index == RETURN else src,
                dst_ref=dst.at[own],
                send_sem=send_sem.at[index],
                recv_sem=recv_sem.at[index],
                device_id=d,
                device_id_type=LOGICAL,
            ).start()

    ret_out[...] = av[...].T
    send_rows(ret_out, ret_in, 1, RETURN)
    own_row = pl.ds(me, 1)
    own_copy = pltpu.make_async_copy(ret_out.at[own_row], ret_in.at[own_row], local_sem.at[RETURN])
    own_copy.start()
    assemble_force()
    send_rows(nrow, nall, 2, NORM)
    finish(ORDER[LAST])
    whole(ret_out, ret_in, 1, RETURN).wait_recv()
    own_copy.wait()
    back = ret_in[...].T
    at_home = [lanes(back[8 * i : 8 * i + 8, :], home_rows) for i in range(6)]

    def tangent(m, j):
        row = (1 + j) * 6 + m
        return at_home[row // 8][row % 8 : row % 8 + 1, :]

    diagonal = []
    for i in range(3):
        value = zero
        for k, m in TERMS[i]:
            inner = zero
            for l, j in TERMS[i]:
                inner = inner + grad[l] * tangent(m, j)
            value = value + grad[k] * inner
        diagonal.append(to_nodes(value))
    tile = tiled(diagonal)
    ntile[...] = tile
    halo_out = [near(3 + i, ntile, nhalo.at[i], s, r) for i, (s, r) in enumerate(steps)]
    for copy in halo_out:
        copy.start()

    pltpu.make_async_remote_copy(
        src_ref=nall.at[pl.ds(0, 2 * NDEV - 2)],
        dst_ref=nall.at[pl.ds(0, 2 * NDEV - 2)],
        send_sem=send_sem.at[NORM],
        recv_sem=recv_sem.at[NORM],
        device_id=other,
        device_id_type=LOGICAL,
    ).wait_recv()
    turn = jnp.where(lax.rem(row8, 4) == 0, row8 + 3, row8 - 1)
    square = zero
    load_sum = zero
    low = lax.rem(lane, 64)
    for half in range(2):
        before_z = zero
        for block in range(16):
            value = nall[pl.ds(block * 16 + half, 8, stride=2), :]
            if half == 1:
                load_sum = load_sum + jnp.where(lane == NDEV - 1, value, 0.0)
                value = jnp.where(lane < 64, value, 0.0)
            other = pltpu.roll(sublanes(value, turn), NDEV - 16, axis=1)
            value = value + jnp.where((low < 8) | ((low >= 24) & (low < 32)), other, 0.0)
            plane = pltpu.roll(value, NDEV - 24, axis=1)
            shifted = jnp.where(row8 < 4, pltpu.roll(before_z, 4, axis=0), pltpu.roll(plane, 4, axis=0))
            before_z = plane
            value = jnp.where(low < 16, value + shifted, 0.0)
            whole_residual[half, pl.ds(block * 8, 8), :] = value
            square = square + value * value
    ratio = jnp.sqrt(jnp.sum(square, keepdims=True) / jnp.sum(load_sum, keepdims=True))
    norm_ref[...] = jnp.broadcast_to(ratio, (8, NDEV))

    for copy in halo_out:
        copy.wait()
    above = jnp.where(sub > 0, 1.0, 0.0).astype(F32)
    node = jnp.where(lane < 16, tile, 0.0)
    node = node + jnp.where(lane < 8, pltpu.roll(nhalo[0], NDEV - 16, axis=1), 0.0)
    node = node + jnp.where(lane < 16, pltpu.roll(nhalo[1], NDEV - 24, axis=1) * above, 0.0)
    node = node + jnp.where(lane < 8, pltpu.roll(nhalo[2], NDEV - 40, axis=1) * above, 0.0)
    pair = whole_residual[0, pl.ds(me, 1), :]
    residual = jnp.concatenate([pair, pltpu.roll(pair, 64, axis=1), whole_residual[1, pl.ds(me, 1), :]], axis=0)
    moved = dtile[0:3, :] + residual / jnp.maximum(node[0:3], FLOOR)
    for i in range(3):
        for y in range(2):
            displaced_ref[i, 0, y : y + 1, :] = moved[i : i + 1, 8 * y : 8 * y + 8]
            residual_ref[i, 0, y : y + 1, :] = residual[i : i + 1, 8 * y : 8 * y + 8]

    for chunk in range(CASES):
        whole(sends[chunk], recvs[chunk], CHUNKS[chunk], chunk).wait_send()
    whole(ret_out, ret_in, 1, RETURN).wait_send()
    pltpu.make_async_remote_copy(
        src_ref=nall.at[pl.ds(0, 2 * NDEV - 2)],
        dst_ref=nall.at[pl.ds(0, 2 * NDEV - 2)],
        send_sem=send_sem.at[NORM],
        recv_sem=recv_sem.at[NORM],
        device_id=other,
        device_id_type=LOGICAL,
    ).wait_send()


def write_out(new_vmem, displaced_vmem, residual_vmem, norm_vmem, new_ref, displaced_ref, residual_ref, norm_ref, sem):
    copies = []
    for case in range(CASES):
        span = pl.ds(case * CASE_ROWS, CASE_ROWS)
        copies.append((new_vmem.at[span], new_ref.at[span]))
    copies += [(displaced_vmem, displaced_ref), (residual_vmem, residual_ref), (norm_vmem.at[pl.ds(0, 1)], norm_ref)]
    copies = [pltpu.make_async_copy(src, dst, sem.at[i]) for i, (src, dst) in enumerate(copies)]
    for copy in copies:
        copy.start()
    for copy in copies:
        copy.wait()


def per_device(displacement, load, home_slot, micro_state, state_slot, phases, phase_moduli):
    floats, ints = tables()
    vmem = pl.BlockSpec(memory_space=pltpu.VMEM)
    hbm = pl.BlockSpec(memory_space=pltpu.HBM)
    buffers = [pltpu.VMEM((NDEV * rows, NDEV), F32) for rows in CHUNKS]
    cells = pltpu.VMEM((3 * CELLS, 8, NDEV), F32)
    dma = pltpu.SemaphoreType.DMA
    arguments = (
        displacement,
        load,
        home_slot.reshape(1, NDEV),
        state_slot.reshape(1, NDEV),
        phase_moduli,
        jnp.asarray(floats),
        jnp.asarray(ints),
        micro_state.reshape(ROWS, NDEV),
        phases,
    )
    results = pl.pallas_call(
        kernel,
        out_shape=(
            pltpu.VMEM((ROWS, NDEV), F32),
            pltpu.VMEM(displacement.shape, F32),
            pltpu.VMEM(displacement.shape, F32),
            pltpu.VMEM((8, NDEV), F32),
        ),
        in_specs=[hbm] * 9,
        out_specs=(vmem,) * 4,
        scratch_shapes=[
            pltpu.VMEM(displacement.shape, F32),
            pltpu.VMEM(load.shape, F32),
            pltpu.VMEM((1, NDEV), jnp.int32),
            pltpu.VMEM((1, NDEV), jnp.int32),
            pltpu.VMEM(phase_moduli.shape, F32),
            pltpu.VMEM(floats.shape, F32),
            pltpu.VMEM(ints.shape, jnp.int32),
            pltpu.VMEM((ROWS + 72, NDEV), F32),
            pltpu.VMEM((VOX + 8, NDEV), jnp.int32),
            *buffers,
            *buffers,
            pltpu.VMEM((ROWS + 72, NDEV), F32),
            pltpu.VMEM((CELLS, 8, NDEV), F32),
            pltpu.VMEM((CELLS, 8, NDEV), F32),
            cells,
            cells,
            cells,
            cells,
            pltpu.VMEM((6 * CELLS, 8, NDEV), F32),
            pltpu.VMEM((2, 8, NDEV), F32),
            pltpu.VMEM((NDEV, NDEV), F32),
            pltpu.VMEM((NDEV, NDEV), F32),
            pltpu.VMEM((NDEV, NDEV), F32),
            pltpu.VMEM((8, NDEV), F32),
            pltpu.VMEM((4, 8, NDEV), F32),
            pltpu.VMEM((8, NDEV), F32),
            pltpu.VMEM((3, 8, NDEV), F32),
            pltpu.VMEM((2, NDEV), F32),
            pltpu.VMEM((2 * NDEV, NDEV), F32),
            pltpu.VMEM((2, NDEV, NDEV), F32),
            dma((7,)),
            dma((CASES,)),
            dma,
            dma((CASES + 1,)),
            dma((CASES + 2,)),
            dma((CASES + 2,)),
            dma((6,)),
            dma((6,)),
        ],
        compiler_params=pltpu.CompilerParams(
            collective_id=1, has_side_effects=True, vmem_limit_bytes=48 * 1024 * 1024
        ),
    )(*[pltpu.with_memory_space_constraint(x, pltpu.HBM) for x in arguments])
    new_state, displaced, residual, norm = pl.pallas_call(
        write_out,
        out_shape=tuple(pltpu.HBM(shape, F32) for shape in (results[0].shape, *[displacement.shape] * 2, (1, NDEV))),
        in_specs=[vmem] * 4,
        out_specs=(hbm,) * 4,
        scratch_shapes=[dma((CASES + 3,))],
        compiler_params=pltpu.CompilerParams(vmem_limit_bytes=4 * 1024 * 1024),
    )(*results)
    return new_state.reshape(CASES, 3, VOX, NDEV), displaced, residual, norm[0, 0]


def solution(mesh):
    both = ("sub", "rve")
    return jax.shard_map(
        per_device,
        mesh=mesh,
        in_specs=(
            P(None, "sub", "rve", None),
            P(None, "sub", "rve", None),
            P(both),
            P(None, None, None, both),
            P(both),
            P(None, both),
            P(),
        ),
        out_specs=(
            P(None, None, None, both),
            P(None, "sub", "rve", None),
            P(None, "sub", "rve", None),
            P(),
        ),
        check_vma=False,
    )
```

```python
import itertools
import math

import jax
import jax.numpy as jnp
import numpy as np
from jax import lax
from jax.experimental import pallas as pl
from jax.experimental.pallas import tpu as pltpu
from jax.sharding import PartitionSpec as P

R = 6
VOX = 216
CASES = 7
STAB = 0.1
FLOOR = 1.0
NDEV = 128
NRVE = 4
NSUB = 32
ROWS = CASES * 3 * VOX
CASE_ROWS = 3 * VOX
CHUNKS = (6, 5, 5, 5, 5, 5, 5)
FIRST = (0, 6, 11, 16, 21, 26, 31)
LAST = len(CHUNKS) - 1
ORDER = (1, 2, 0, 3, 4, 5, 6)
MACRO = 2
STRAIN_ROW = 3 * CASE_ROWS
STRESS_ROW = 7 * CASE_ROWS + 8
RESULT = LAST + 1
CELLS = 36
LOGICAL = pl.DeviceIdType.LOGICAL
F32 = jnp.float32
TERMS = (((0, 0), (2, 4), (1, 5)), ((1, 1), (2, 3), (0, 5)), ((2, 2), (1, 3), (0, 4)))
ENTRIES = [(m, m) for m in range(6)]
ENTRIES += [(min(t[0][1], t[1][1]), max(t[0][1], t[1][1])) for i in range(3) for t in itertools.combinations(TERMS[i], 2)]


def tables():
    offset = 0.5 / math.sqrt(3.0)
    places = (0.5 - offset, 0.5 + offset)
    slopes = np.zeros((3, 8, NDEV), np.float32)
    for g in range(NDEV):
        q = g % 8
        at = (places[q % 2], places[q // 2 % 2], places[q // 4])
        for a in range(8):
            bits = (a % 2, a // 2 % 2, a // 4)
            w = [at[k] if bits[k] else 1.0 - at[k] for k in range(3)]
            s = [1.0 if bits[k] else -1.0 for k in range(3)]
            slopes[0, a, g] = s[0] * w[1] * w[2]
            slopes[1, a, g] = w[0] * s[1] * w[2]
            slopes[2, a, g] = w[0] * w[1] * s[2]
    mask = np.zeros((8, NDEV), np.float32)
    pick = np.zeros((8, NDEV), np.int32)
    for n in range(48):
        nz, ny, nx = n // 24, n // 8 % 3, n % 8
        for a in range(8):
            ax, ay, az = a % 2, a // 2 % 2, a // 4
            ly = ny - ay
            if az == nz and 0 <= ly < 2:
                mask[a, n] = 1.0
                pick[a, n] = (ly * 8 + (nx - ax) % 8) * 8
    corner = np.zeros((8, NDEV), np.int32)
    for g in range(NDEV):
        ly, ex = g // 64, g // 8 % 8
        for a in range(8):
            ax, ay, az = a % 2, a // 2 % 2, a // 4
            corner[a, g] = az * 24 + (ly + ay) * 8 + (ex + ax) % 8
    own = np.zeros((8, NDEV), np.int32)
    for n in range(16):
        ny, nx = n // 8, n % 8
        for a in range(8):
            ax, ay = a % 2, a // 2 % 2
            own[a, n] = ((1 - ny if ay else ny) * 8 + (nx - ax) % 8) * 8
    floats = np.concatenate([slopes.reshape(24, NDEV), mask], axis=0)
    ints = np.concatenate([pick, corner, own], axis=0)
    return floats, ints


def base_of(position):
    return position * CASE_ROWS + 8 * ((position + 3) // 6)


def around(step):
    return min(step, 4 - step)


SPREAD = [((i // 16 + i) % 4, (i // 4 + i) % 4, c, i % 4) for c in range(2) for i in range(64)][1:]
FARTHEST = sorted(SPREAD, key=lambda o: -(around(o[0]) + around(o[1]) + around(o[3]) + 0.3 * o[2]))


def lanes(x, index):
    return jnp.take_along_axis(x, index, axis=1, mode="promise_in_bounds")


def sublanes(x, index):
    return jnp.take_along_axis(x, index, axis=0, mode="promise_in_bounds")


def spread(row):
    return jnp.broadcast_to(row, (8, NDEV))


def inverse(target):
    column = jnp.broadcast_to(target, (NDEV, NDEV)).T
    lane = lax.broadcasted_iota(jnp.int32, (NDEV, NDEV), 1)
    row = lax.broadcasted_iota(jnp.int32, (NDEV, NDEV), 0)
    return jnp.sum(jnp.where(column == lane, row, 0).astype(F32), axis=0, keepdims=True).astype(jnp.int32)


def kernel(
    disp_hbm, load_hbm, home_hbm, state_hbm, moduli_hbm, float_hbm, int_hbm, micro_ref, phase_ref,
    new_ref, displaced_ref, residual_ref, norm_ref,
    disp_ref, load_ref, home_ref, state_slot_ref, moduli_ref, float_ref, int_ref, xin, ph, send0, send1, send2, send3, send4, send5, send6, recv0, recv1, recv2, recv3, recv4, recv5, recv6,
    nat, lam, mu, w, p0, p1, ap, sig, keep, av, rows_out, rows_in, dtile, dhalo, home_near, spare, whole_residual,
    small_sem, in_sem, ph_sem, local_sem, send_sem, recv_sem, near_send, near_recv,
):
    sub, rve = lax.axis_index("sub"), lax.axis_index("rve")
    me = sub * NRVE + rve
    sends = (send0, send1, send2, send3, send4, send5, send6)
    recvs = (recv0, recv1, recv2, recv3, recv4, recv5, recv6)
    along_z = [lax.rem(sub // 8 + i, 4) * 32 for i in range(4)]
    along_y = [lax.rem(lax.rem(sub // 2, 4) + i, 4) * 8 for i in range(4)]
    along_c = [lax.rem(lax.rem(sub, 2) + i, 2) * 4 for i in range(2)]
    along_x = [lax.rem(rve + i, 4) for i in range(4)]

    def others(order):
        for z, y, c, x in order:
            yield along_z[z] + along_y[y] + (along_c[c] + along_x[x])

    other = along_z[0] + along_y[0] + (along_c[0] + along_x[1])

    barrier = pltpu.get_barrier_semaphore()

    for d in others(FARTHEST):
        pl.semaphore_signal(barrier, inc=1, device_id=d, device_id_type=LOGICAL)

    small = []
    pairs = (
        (state_hbm, state_slot_ref), (home_hbm, home_ref), (disp_hbm, disp_ref), (load_hbm, load_ref),
        (moduli_hbm, moduli_ref), (float_hbm, float_ref), (int_hbm, int_ref),
    )
    for i, (src, dst) in enumerate(pairs):
        small.append(pltpu.make_async_copy(src, dst, small_sem.at[i]))
        small[-1].start()

    loads = []
    for position, case in enumerate(ORDER):
        copy = pltpu.make_async_copy(
            micro_ref.at[pl.ds(case * CASE_ROWS, CASE_ROWS)],
            xin.at[pl.ds(base_of(position), CASE_ROWS)],
            in_sem.at[position],
        )
        copy.start()
        loads.append(copy)
    phase_load = pltpu.make_async_copy(phase_ref, ph.at[pl.ds(0, VOX)], ph_sem)
    phase_load.start()

    for copy in small:
        copy.wait()
    dtile[...] = jnp.zeros((8, NDEV), F32)
    for i in range(3):
        for y in range(2):
            dtile[i : i + 1, 8 * y : 8 * y + 8] = disp_ref[i, 0, y : y + 1, :]

    home_dev = lax.shift_right_logical(home_ref[...], 7)
    state_index = spread(inverse(lax.shift_right_logical(state_slot_ref[...], 7)))
    home_index = spread(inverse(home_dev))

    def prepare(chunk, row):
        parts = []
        for i in range(16):
            at = (FIRST[chunk] + row) * NDEV + 8 * i
            block = xin[pl.ds(at, 8), :]
            if at == STRAIN_ROW:
                block = lanes(block, home_index)
            elif at != STRESS_ROW:
                block = lanes(block, state_index)
            parts.append(block)
        sends[chunk][pl.ds(row, NDEV, stride=CHUNKS[chunk]), :] = jnp.concatenate(parts, axis=0).T

    def prepare_chunk(chunk):
        for row in range(CHUNKS[chunk]):
            prepare(chunk, row)

    def send_chunk(chunk):
        rows = CHUNKS[chunk]
        own = pl.ds(me * rows, rows)
        for d in others(SPREAD):
            pltpu.make_async_remote_copy(
                src_ref=sends[chunk].at[pl.ds(d * rows, rows)],
                dst_ref=recvs[chunk].at[own],
                send_sem=send_sem.at[chunk],
                recv_sem=recv_sem.at[chunk],
                device_id=d,
                device_id_type=LOGICAL,
            ).start()
        pltpu.make_async_copy(sends[chunk].at[own], recvs[chunk].at[own], local_sem.at[chunk]).start()

    def whole(src, dst, rows, index):
        return pltpu.make_async_remote_copy(
            src_ref=src.at[pl.ds(0, (NDEV - 1) * rows)],
            dst_ref=dst.at[pl.ds(0, (NDEV - 1) * rows)],
            send_sem=send_sem.at[index],
            recv_sem=recv_sem.at[index],
            device_id=other,
            device_id_type=LOGICAL,
        )

    for position in (0, 1):
        loads[position].wait()
    prepare_chunk(0)

    pl.semaphore_wait(barrier, NDEV - 1)

    def near(index, src, dst, dsub, drve):
        to_sub = lax.rem(sub + dsub + NSUB, NSUB)
        to_rve = lax.rem(rve + drve + NRVE, NRVE)
        return pltpu.make_async_remote_copy(
            src_ref=src,
            dst_ref=dst,
            send_sem=near_send.at[index],
            recv_sem=near_recv.at[index],
            device_id=to_sub * NRVE + to_rve,
            device_id_type=LOGICAL,
        )

    steps = ((0, 1), (1, 0), (1, 1))
    halo_in = [near(i, dtile, dhalo.at[i], -s, -r) for i, (s, r) in enumerate(steps)]
    halo_in += [near(3 + i, home_ref, home_near.at[i], s, r) for i, (s, r) in enumerate(steps)]
    for copy in halo_in:
        copy.start()
    send_chunk(0)
    loads[2].wait()
    prepare_chunk(1)
    send_chunk(1)

    for copy in halo_in:
        copy.wait()
    lane = lax.broadcasted_iota(jnp.int32, (8, NDEV), 1)
    row8 = lax.broadcasted_iota(jnp.int32, (8, NDEV), 0)
    below = jnp.where(sub < NSUB - 1, 1.0, 0.0).astype(F32)
    extended = dtile[...]
    extended = jnp.where((lane >= 16) & (lane < 24), pltpu.roll(dhalo[0], 16, axis=1), extended)
    extended = jnp.where((lane >= 24) & (lane < 40), pltpu.roll(dhalo[1], 24, axis=1) * below, extended)
    extended = jnp.where((lane >= 40) & (lane < 48), pltpu.roll(dhalo[2], 40, axis=1) * below, extended)
    slope = [jnp.zeros((8, NDEV), F32) for _ in range(3)]
    for a in range(8):
        value = lanes(extended, spread(int_ref[8 + a : 9 + a, :]))
        for k in range(3):
            slope[k] = slope[k] + float_ref[8 * k + a : 8 * k + a + 1, :] * value
    s0, s1, s2 = slope
    strains = [
        s0[0:1], s1[1:2], s2[2:3],
        s2[1:2] + s1[2:3], s2[0:1] + s0[2:3], s1[0:1] + s0[1:2],
    ]
    strain_rows = jnp.zeros((8, NDEV), F32)
    for m in range(6):
        strain_rows = jnp.where(row8 == m, spread(strains[m]), strain_rows)
    xin[pl.ds(STRAIN_ROW, 8), :] = strain_rows
    for chunk in range(MACRO, LAST):
        loads[chunk + 1].wait()
        prepare_chunk(chunk)
        send_chunk(chunk)
    xin[pl.ds(STRESS_ROW + 8, 56), :] = jnp.zeros((56, NDEV), F32)

    phase_load.wait()
    ph[pl.ds(VOX, 8), :] = jnp.zeros((8, NDEV), jnp.int32)
    inside = row8 < R
    moduli = [
        [jnp.broadcast_to(moduli_ref[which : which + 1, p : p + 1], (8, NDEV)) for p in range(3)] for which in range(2)
    ]

    @pl.loop(0, CELLS)
    def _(cell):
        label = ph[pl.ds(cell * R, 8), :]
        for which, out in ((0, lam), (1, mu)):
            value = jnp.where(
                label == 0,
                moduli[which][0],
                jnp.where(label == 1, moduli[which][1], moduli[which][2]),
            )
            out[cell] = jnp.where(inside, value, 0.0)

    av[...] = jnp.zeros((NDEV, NDEV), F32)
    up = jnp.where(row8 < 5, row8 + 1, jnp.where(row8 == 5, 0, row8))
    down = jnp.where(row8 == 0, 5, jnp.where(row8 < 6, row8 - 1, row8))

    def receive(chunk):
        rows = CHUNKS[chunk]
        own = pl.ds(me * rows, rows)
        whole(sends[chunk], recvs[chunk], rows, chunk).wait_recv()
        pltpu.make_async_copy(sends[chunk].at[own], recvs[chunk].at[own], local_sem.at[chunk]).wait()
        for row in range(rows):
            block = recvs[chunk][pl.ds(row, NDEV, stride=rows), :]
            nat[pl.ds((FIRST[chunk] + row) * NDEV, NDEV), :] = block.T

    zero = jnp.zeros((8, NDEV), F32)

    def stress_at(src, a, b, applied):
        following = lax.rem(a + 1, R)
        g = []
        for i in range(3):
            here = src[i * CELLS + a * R + b]
            g.append(
                (
                    src[i * CELLS + following * R + b] - here,
                    src[i * CELLS + a * R + (b + 1) % R] - here,
                    sublanes(here, up) - here,
                )
            )
        eps = [g[0][0], g[1][1], g[2][2], g[1][2] + g[2][1], g[0][2] + g[2][0], g[0][1] + g[1][0]]
        if applied is not None:
            eps = [eps[m] + applied[m] for m in range(6)]
        cell = a * R + b
        first, second = lam[cell], mu[cell]
        volume = first * (eps[0] + eps[1] + eps[2])
        twice = second + second
        stress = [volume + twice * eps[m] for m in range(3)] + [second * eps[m] for m in range(3, 6)]
        return stress, eps

    def stresses(src, applied):
        def body(a, total):
            total = list(total)
            for b in range(R):
                stress, _ = stress_at(src, a, b, applied)
                for m in range(6):
                    sig[m * CELLS + a * R + b] = stress[m]
                    total[m] = total[m] + stress[m]
            return tuple(total)

        return lax.fori_loop(0, R, body, (zero,) * 6)

    voigt = ((0, 5, 4), (5, 1, 3), (4, 3, 2))

    def force_at(src, a, b):
        before = lax.rem(a + R - 1, R)
        cell = a * R + b
        here = [sig[m * CELLS + cell] for m in range(6)]
        out = []
        for i in range(3):
            total = sig[voigt[0][i] * CELLS + before * R + b] - here[voigt[0][i]]
            total = total + (sig[voigt[1][i] * CELLS + a * R + (b + R - 1) % R] - here[voigt[1][i]])
            last = here[voigt[2][i]]
            total = total + (sublanes(last, down) - last)
            out.append(total + STAB * src[i * CELLS + cell])
        return out

    def across(x):
        return spread(jnp.sum(x, axis=0, keepdims=True))

    def finish(case):
        alpha0, alpha1 = keep[0], keep[1]

        @pl.loop(0, R)
        def _(a):
            for i in range(3):
                to = case * CASE_ROWS + i * VOX + a * (R * R)
                for b in range(R):
                    at = i * CELLS + a * R + b
                    value = w[at] + alpha0 * p0[at] + alpha1 * p1[at]
                    new_ref[pl.ds(to + b * R, R), :] = value[0:R, :]

    for i in range(3):
        for y in range(2):
            dhalo[3, i : i + 1, 8 * y : 8 * y + 8] = load_ref[i, 0, y : y + 1, :]
    home_rows = spread(home_dev)
    grad = [float_ref[8 * k : 8 * k + 8, :] for k in range(3)]

    def to_nodes(value):
        for step in (1, 2, 4):
            value = value + pltpu.roll(value, NDEV - step, axis=1)
        value = lanes(value, int_ref[0:8, :]) * (float_ref[24:32, :] * 0.125)
        return jnp.sum(value, axis=0, keepdims=True)

    def tiled(rows):
        tile = zero
        for r, value in enumerate(rows):
            tile = jnp.where(row8 == r, spread(value), tile)
        return tile

    def residual_part():
        stress = lanes(nat[pl.ds(STRESS_ROW, 8), :], home_rows)
        rows = []
        for i in range(3):
            value = zero
            for k, m in TERMS[i]:
                value = value + grad[k] * spread(stress[m : m + 1, :])
            rows.append(to_nodes(value))
        load_rows = jnp.where((lane < 16) & (row8 < 3), dhalo[3], 0.0)
        load_square = jnp.sum(load_rows * load_rows, keepdims=True)
        part = load_rows - tiled(rows)
        first_row = part[0:1] + pltpu.roll(part[1:2], 64, axis=1)
        second_row = jnp.where(lane[0:1] == 63, jnp.broadcast_to(load_square, (1, NDEV)), part[2:3])
        return spread(first_row), spread(second_row)

    def case_body(position, carry):
        for chunk in range(CASES):

            @pl.when(position == chunk)
            def _():
                receive(chunk)

        plain = (position + 3) // 6
        case = plain * position + (1 - plain) * lax.rem(position + 1, 3)
        macro = nat[pl.ds(STRAIN_ROW, 8), :]
        applied = []
        for m in range(6):
            unit = jnp.where(case == m + 1, 1.0, 0.0).astype(F32)
            applied.append(jnp.where(position == MACRO, spread(macro[m : m + 1, :]), unit))

        @pl.loop(0, R)
        def _(a):
            for i in range(3):
                at = base_of(position) + i * VOX + a * (R * R)
                for b in range(R):
                    w[i * CELLS + a * R + b] = jnp.where(inside, nat[pl.ds(at + b * R, 8), :], 0.0)

        total0 = stresses(w, applied)

        def first(a, rr):
            for b in range(R):
                force = force_at(w, a, b)
                for i in range(3):
                    value = -force[i]
                    p0[i * CELLS + a * R + b] = value
                    force[i] = value * value
                rr = rr + (force[0] + (force[1] + force[2]))
            return rr

        rr = across(lax.fori_loop(0, R, first, zero))
        total1 = stresses(p0, None)

        def second(a, curve):
            for b in range(R):
                force = force_at(p0, a, b)
                for i in range(3):
                    ap[i * CELLS + a * R + b] = force[i]
                    force[i] = p0[i * CELLS + a * R + b] * force[i]
                curve = curve + (force[0] + (force[1] + force[2]))
            return curve

        alpha0 = rr / across(lax.fori_loop(0, R, second, zero))

        def reduce(a, total):
            total = list(total)
            for j in range(3 * R):
                at = a * (3 * R) + j
                value = p0[at] - alpha0 * ap[at]
                p1[at] = value
                total[j % 6] = total[j % 6] + value * value
            return tuple(total)

        parts = lax.fori_loop(0, R, reduce, (zero,) * 6)
        rn = across(((parts[0] + parts[1]) + (parts[2] + parts[3])) + (parts[4] + parts[5]))
        beta = rn / rr

        @pl.loop(0, R)
        def _(a):
            for j in range(3 * R):
                at = a * (3 * R) + j
                p1[at] = p1[at] + beta * p0[at]

        def third(a, carried):
            curve, total = carried[0], list(carried[1:])
            for b in range(R):
                stress, eps = stress_at(p1, a, b, None)
                for m in range(6):
                    total[m] = total[m] + stress[m]
                work = [stress[m] * eps[m] for m in range(6)]
                here = [p1[i * CELLS + a * R + b] for i in range(3)]
                kept = STAB * ((here[0] * here[0] + here[1] * here[1]) + here[2] * here[2])
                curve = curve + (((work[0] + work[1]) + (work[2] + work[3])) + ((work[4] + work[5]) + kept))
            return (curve, *total)

        found = lax.fori_loop(0, R, third, (zero,) * 7)
        alpha1 = rn / across(found[0])
        for m in range(6):
            mean = jnp.sum(total0[m] + alpha0 * total1[m] + alpha1 * found[1 + m], axis=0, keepdims=True)
            av[pl.ds(case * 6 + m, 1), :] = mean * (1.0 / VOX)

        keep[0], keep[1] = alpha0, alpha1

        @pl.when(position < LAST)
        def _():
            finish(case)

        @pl.when(position == MACRO)
        def _():
            xin[pl.ds(STRESS_ROW, 8), :] = av[0:8, :]
            prepare_chunk(LAST)
            send_chunk(LAST)

        return carry

    lax.fori_loop(0, CASES, case_body, 0)

    for r, (m, j) in enumerate(ENTRIES):
        entry = av[(1 + j) * 6 + m : (1 + j) * 6 + m + 1, :]
        if m != j:
            entry = entry + av[(1 + m) * 6 + j : (1 + m) * 6 + j + 1, :]
        spare[r : r + 1, :] = entry
    spare[15:16, :] = jnp.zeros((1, NDEV), F32)
    step_back = lax.rem(lane + 3, 4) - lax.rem(lane, 4) + lane
    here = [spare[0:8, :], spare[8:16, :]]
    beside = [lanes(x, step_back) for x in here]
    under = [pltpu.roll(x, NRVE, axis=1) for x in here + beside]
    back_rows = jnp.concatenate([zero] * 8 + here + beside + under, axis=0).T
    first_row, second_row = residual_part()
    for block in range(16):
        rows_out[pl.ds(block * 16, 8, stride=2), :] = first_row
        rows_out[pl.ds(block * 16 + 1, 8, stride=2), :] = back_rows[8 * block : 8 * block + 8, :] + second_row
    own = pl.ds(me * 2, 2)
    for d in others(FARTHEST):
        pltpu.make_async_remote_copy(
            src_ref=rows_out.at[pl.ds(d * 2, 2)],
            dst_ref=rows_in.at[own],
            send_sem=send_sem.at[RESULT],
            recv_sem=recv_sem.at[RESULT],
            device_id=d,
            device_id_type=LOGICAL,
        ).start()
    own_copy = pltpu.make_async_copy(rows_out.at[own], rows_in.at[own], local_sem.at[RESULT])
    own_copy.start()
    finish(ORDER[LAST])
    whole(rows_out, rows_in, 2, RESULT).wait_recv()
    own_copy.wait()
    back = rows_in[pl.ds(1, NDEV, stride=2), :].T
    above = jnp.where(sub > 0, 1.0, 0.0).astype(F32)
    targets = [home_rows] + [spread(lax.shift_right_logical(home_near[b], 7)) for b in range(3)]
    product = {(k, l): grad[k] * grad[l] for k in range(3) for l in range(k, 3)}
    parts = []
    for b in range(4):
        found = [lanes(back[64 + 16 * b + 8 * h : 64 + 16 * b + 8 * h + 8, :], targets[b]) for h in range(2)]
        values = []
        for i in range(3):
            value = zero
            for (k, m), (l, j) in itertools.combinations_with_replacement(TERMS[i], 2):
                r = ENTRIES.index((min(m, j), max(m, j)))
                value = value + product[min(k, l), max(k, l)] * spread(found[r // 8][r % 8 : r % 8 + 1, :])
            values.append(value)
        parts.append(values)
    lower = row8 < 4
    crossing = (lax.rem(row8, 4) >= 2) & (lane >= 64)
    diagonal = []
    for i in range(3):
        inner = jnp.where(lower, parts[0][i], parts[2][i] * above)
        outer = jnp.where(lower, parts[1][i], parts[3][i] * above)
        value = jnp.where(crossing, outer, inner)
        for step in (1, 2, 4):
            value = value + pltpu.roll(value, NDEV - step, axis=1)
        value = lanes(value, int_ref[16:24, :]) * 0.125
        diagonal.append(jnp.sum(value, axis=0, keepdims=True))
    node = tiled(diagonal)

    turn = jnp.where(lax.rem(row8, 4) == 0, row8 + 3, row8 - 1)
    square = zero
    load_sum = zero
    low = lax.rem(lane, 64)
    for half in range(2):
        before_z = zero
        for block in range(16):
            value = rows_in[pl.ds(block * 16 + half, 8, stride=2), :]
            if half == 1:
                load_sum = load_sum + jnp.where(lane == 63, value, 0.0)
                value = jnp.where(lane < 48, value, 0.0)
            before = pltpu.roll(sublanes(value, turn), NDEV - 16, axis=1)
            value = value + jnp.where((low < 8) | ((low >= 24) & (low < 32)), before, 0.0)
            plane = pltpu.roll(value, NDEV - 24, axis=1)
            shifted = jnp.where(row8 < 4, pltpu.roll(before_z, 4, axis=0), pltpu.roll(plane, 4, axis=0))
            before_z = plane
            value = jnp.where(low < 16, value + shifted, 0.0)
            whole_residual[half, pl.ds(block * 8, 8), :] = value
            square = square + value * value
    ratio = jnp.sqrt(jnp.sum(square, keepdims=True) / jnp.sum(load_sum, keepdims=True))
    norm_ref[...] = jnp.broadcast_to(ratio, (8, NDEV))

    pair = whole_residual[0, pl.ds(me, 1), :]
    residual = jnp.concatenate([pair, pltpu.roll(pair, 64, axis=1), whole_residual[1, pl.ds(me, 1), :]], axis=0)
    moved = dtile[0:3, :] + residual / jnp.maximum(node[0:3], FLOOR)
    for i in range(3):
        for y in range(2):
            displaced_ref[i, 0, y : y + 1, :] = moved[i : i + 1, 8 * y : 8 * y + 8]
            residual_ref[i, 0, y : y + 1, :] = residual[i : i + 1, 8 * y : 8 * y + 8]

    for chunk in range(CASES):
        whole(sends[chunk], recvs[chunk], CHUNKS[chunk], chunk).wait_send()
    whole(rows_out, rows_in, 2, RESULT).wait_send()


def write_out(new_vmem, displaced_vmem, residual_vmem, norm_vmem, new_ref, displaced_ref, residual_ref, norm_ref, sem):
    copies = []
    for case in range(CASES):
        span = pl.ds(case * CASE_ROWS, CASE_ROWS)
        copies.append((new_vmem.at[span], new_ref.at[span]))
    copies += [(displaced_vmem, displaced_ref), (residual_vmem, residual_ref), (norm_vmem.at[pl.ds(0, 1)], norm_ref)]
    copies = [pltpu.make_async_copy(src, dst, sem.at[i]) for i, (src, dst) in enumerate(copies)]
    for copy in copies:
        copy.start()
    for copy in copies:
        copy.wait()


def per_device(displacement, load, home_slot, micro_state, state_slot, phases, phase_moduli):
    floats, ints = tables()
    vmem = pl.BlockSpec(memory_space=pltpu.VMEM)
    hbm = pl.BlockSpec(memory_space=pltpu.HBM)
    buffers = [pltpu.VMEM((NDEV * rows, NDEV), F32) for rows in CHUNKS]
    cells = pltpu.VMEM((3 * CELLS, 8, NDEV), F32)
    dma = pltpu.SemaphoreType.DMA
    arguments = (
        displacement,
        load,
        home_slot.reshape(1, NDEV),
        state_slot.reshape(1, NDEV),
        phase_moduli,
        jnp.asarray(floats),
        jnp.asarray(ints),
        micro_state.reshape(ROWS, NDEV),
        phases,
    )
    results = pl.pallas_call(
        kernel,
        out_shape=(
            pltpu.VMEM((ROWS, NDEV), F32),
            pltpu.VMEM(displacement.shape, F32),
            pltpu.VMEM(displacement.shape, F32),
            pltpu.VMEM((8, NDEV), F32),
        ),
        in_specs=[hbm] * 9,
        out_specs=(vmem,) * 4,
        scratch_shapes=[
            pltpu.VMEM(displacement.shape, F32),
            pltpu.VMEM(load.shape, F32),
            pltpu.VMEM((1, NDEV), jnp.int32),
            pltpu.VMEM((1, NDEV), jnp.int32),
            pltpu.VMEM(phase_moduli.shape, F32),
            pltpu.VMEM(floats.shape, F32),
            pltpu.VMEM(ints.shape, jnp.int32),
            pltpu.VMEM((ROWS + 72, NDEV), F32),
            pltpu.VMEM((VOX + 8, NDEV), jnp.int32),
            *buffers,
            *buffers,
            pltpu.VMEM((ROWS + 72, NDEV), F32),
            pltpu.VMEM((CELLS, 8, NDEV), F32),
            pltpu.VMEM((CELLS, 8, NDEV), F32),
            cells,
            cells,
            cells,
            cells,
            pltpu.VMEM((6 * CELLS, 8, NDEV), F32),
            pltpu.VMEM((2, 8, NDEV), F32),
            pltpu.VMEM((NDEV, NDEV), F32),
            pltpu.VMEM((2 * NDEV, NDEV), F32),
            pltpu.VMEM((2 * NDEV, NDEV), F32),
            pltpu.VMEM((8, NDEV), F32),
            pltpu.VMEM((4, 8, NDEV), F32),
            pltpu.VMEM((3, 1, NDEV), jnp.int32),
            pltpu.VMEM((16, NDEV), F32),
            pltpu.VMEM((2, NDEV, NDEV), F32),
            dma((7,)),
            dma((CASES,)),
            dma,
            dma((CASES + 1,)),
            dma((CASES + 1,)),
            dma((CASES + 1,)),
            dma((6,)),
            dma((6,)),
        ],
        compiler_params=pltpu.CompilerParams(
            collective_id=1, has_side_effects=True, vmem_limit_bytes=48 * 1024 * 1024
        ),
    )(*[pltpu.with_memory_space_constraint(x, pltpu.HBM) for x in arguments])
    new_state, displaced, residual, norm = pl.pallas_call(
        write_out,
        out_shape=tuple(pltpu.HBM(shape, F32) for shape in (results[0].shape, *[displacement.shape] * 2, (1, NDEV))),
        in_specs=[vmem] * 4,
        out_specs=(hbm,) * 4,
        scratch_shapes=[dma((CASES + 3,))],
        compiler_params=pltpu.CompilerParams(vmem_limit_bytes=4 * 1024 * 1024),
    )(*results)
    return new_state.reshape(CASES, 3, VOX, NDEV), displaced, residual, norm[0, 0]


def solution(mesh):
    both = ("sub", "rve")
    return jax.shard_map(
        per_device,
        mesh=mesh,
        in_specs=(
            P(None, "sub", "rve", None),
            P(None, "sub", "rve", None),
            P(both),
            P(None, None, None, both),
            P(both),
            P(None, both),
            P(),
        ),
        out_specs=(
            P(None, None, None, both),
            P(None, "sub", "rve", None),
            P(None, "sub", "rve", None),
            P(),
        ),
        check_vma=False,
    )
```

```python
import itertools
import math

import jax
import jax.numpy as jnp
import numpy as np
from jax import lax
from jax.experimental import pallas as pl
from jax.experimental.pallas import tpu as pltpu
from jax.sharding import PartitionSpec as P

R = 6
VOX = 216
CASES = 7
STAB = 0.1
FLOOR = 1.0
NDEV = 128
NRVE = 4
NSUB = 32
ROWS = CASES * 3 * VOX
CASE_ROWS = 3 * VOX
CHUNKS = (6, 5, 5, 5, 5, 5, 5)
FIRST = (0, 6, 11, 16, 21, 26, 31)
LAST = len(CHUNKS) - 1
ORDER = (1, 2, 0, 3, 4, 5, 6)
MACRO = 2
STRAIN_ROW = 3 * CASE_ROWS
STRESS_ROW = 7 * CASE_ROWS + 8
RESULT = LAST + 1
CELLS = 36
LOGICAL = pl.DeviceIdType.LOGICAL
F32 = jnp.float32
TERMS = (((0, 0), (2, 4), (1, 5)), ((1, 1), (2, 3), (0, 5)), ((2, 2), (1, 3), (0, 4)))
ENTRIES = [(m, m) for m in range(6)]
ENTRIES += [(min(t[0][1], t[1][1]), max(t[0][1], t[1][1])) for i in range(3) for t in itertools.combinations(TERMS[i], 2)]


def tables():
    offset = 0.5 / math.sqrt(3.0)
    places = (0.5 - offset, 0.5 + offset)
    slopes = np.zeros((3, 8, NDEV), np.float32)
    for g in range(NDEV):
        q = g % 8
        at = (places[q % 2], places[q // 2 % 2], places[q // 4])
        for a in range(8):
            bits = (a % 2, a // 2 % 2, a // 4)
            w = [at[k] if bits[k] else 1.0 - at[k] for k in range(3)]
            s = [1.0 if bits[k] else -1.0 for k in range(3)]
            slopes[0, a, g] = s[0] * w[1] * w[2]
            slopes[1, a, g] = w[0] * s[1] * w[2]
            slopes[2, a, g] = w[0] * w[1] * s[2]
    mask = np.zeros((8, NDEV), np.float32)
    pick = np.zeros((8, NDEV), np.int32)
    for n in range(48):
        nz, ny, nx = n // 24, n // 8 % 3, n % 8
        for a in range(8):
            ax, ay, az = a % 2, a // 2 % 2, a // 4
            ly = ny - ay
            if az == nz and 0 <= ly < 2:
                mask[a, n] = 1.0
                pick[a, n] = (ly * 8 + (nx - ax) % 8) * 8
    corner = np.zeros((8, NDEV), np.int32)
    for g in range(NDEV):
        ly, ex = g // 64, g // 8 % 8
        for a in range(8):
            ax, ay, az = a % 2, a // 2 % 2, a // 4
            corner[a, g] = az * 24 + (ly + ay) * 8 + (ex + ax) % 8
    own = np.zeros((8, NDEV), np.int32)
    for n in range(16):
        ny, nx = n // 8, n % 8
        for a in range(8):
            ax, ay = a % 2, a // 2 % 2
            own[a, n] = ((1 - ny if ay else ny) * 8 + (nx - ax) % 8) * 8
    floats = np.concatenate([slopes.reshape(24, NDEV), mask], axis=0)
    ints = np.concatenate([pick, corner, own], axis=0)
    return floats, ints


def base_of(position):
    return position * CASE_ROWS + 8 * ((position + 3) // 6)


def around(step):
    return min(step, 4 - step)


SPREAD = [((i // 16 + i) % 4, (i // 4 + i) % 4, c, i % 4) for c in range(2) for i in range(64)][1:]
FARTHEST = sorted(SPREAD, key=lambda o: -(around(o[0]) + around(o[1]) + around(o[3]) + 0.3 * o[2]))


def lanes(x, index):
    return jnp.take_along_axis(x, index, axis=1, mode="promise_in_bounds")


def sublanes(x, index):
    return jnp.take_along_axis(x, index, axis=0, mode="promise_in_bounds")


def spread(row):
    return jnp.broadcast_to(row, (8, NDEV))


def inverse(target):
    column = jnp.broadcast_to(target, (NDEV, NDEV)).T
    lane = lax.broadcasted_iota(jnp.int32, (NDEV, NDEV), 1)
    row = lax.broadcasted_iota(jnp.int32, (NDEV, NDEV), 0)
    return jnp.sum(jnp.where(column == lane, row, 0).astype(F32), axis=0, keepdims=True).astype(jnp.int32)


def kernel(
    disp_hbm, load_hbm, home_hbm, state_hbm, moduli_hbm, float_hbm, int_hbm, micro_ref, phase_ref,
    new_ref, displaced_ref, residual_ref, norm_ref,
    disp_ref, load_ref, home_ref, state_slot_ref, moduli_ref, float_ref, int_ref, xin, ph, send0, send1, send2, send3, send4, send5, send6, recv0, recv1, recv2, recv3, recv4, recv5, recv6,
    nat, lam, mu, w, p0, p1, ap, sig, keep, av, rows_out, rows_in, dtile, dhalo, home_near, spare, whole_residual,
    small_sem, in_sem, ph_sem, local_sem, send_sem, recv_sem, near_send, near_recv,
):
    sub, rve = lax.axis_index("sub"), lax.axis_index("rve")
    me = sub * NRVE + rve
    sends = (send0, send1, send2, send3, send4, send5, send6)
    recvs = (recv0, recv1, recv2, recv3, recv4, recv5, recv6)
    along_z = [lax.rem(sub // 8 + i, 4) * 32 for i in range(4)]
    along_y = [lax.rem(lax.rem(sub // 2, 4) + i, 4) * 8 for i in range(4)]
    along_c = [lax.rem(lax.rem(sub, 2) + i, 2) * 4 for i in range(2)]
    along_x = [lax.rem(rve + i, 4) for i in range(4)]

    def others(order):
        for z, y, c, x in order:
            yield along_z[z] + along_y[y] + (along_c[c] + along_x[x])

    other = along_z[0] + along_y[0] + (along_c[0] + along_x[1])

    barrier = pltpu.get_barrier_semaphore()

    for d in others(FARTHEST):
        pl.semaphore_signal(barrier, inc=1, device_id=d, device_id_type=LOGICAL)

    small = []
    pairs = (
        (state_hbm, state_slot_ref), (home_hbm, home_ref), (disp_hbm, disp_ref), (load_hbm, load_ref),
        (moduli_hbm, moduli_ref), (float_hbm, float_ref), (int_hbm, int_ref),
    )
    for i, (src, dst) in enumerate(pairs):
        small.append(pltpu.make_async_copy(src, dst, small_sem.at[i]))
        small[-1].start()

    loads = []
    for position, case in enumerate(ORDER):
        copy = pltpu.make_async_copy(
            micro_ref.at[pl.ds(case * CASE_ROWS, CASE_ROWS)],
            xin.at[pl.ds(base_of(position), CASE_ROWS)],
            in_sem.at[position],
        )
        copy.start()
        loads.append(copy)
    phase_load = pltpu.make_async_copy(phase_ref, ph.at[pl.ds(0, VOX)], ph_sem)
    phase_load.start()

    for copy in small:
        copy.wait()
    dtile[...] = jnp.zeros((8, NDEV), F32)
    for i in range(3):
        for y in range(2):
            dtile[i : i + 1, 8 * y : 8 * y + 8] = disp_ref[i, 0, y : y + 1, :]

    home_dev = lax.shift_right_logical(home_ref[...], 7)
    state_index = spread(inverse(lax.shift_right_logical(state_slot_ref[...], 7)))
    home_index = spread(inverse(home_dev))

    def prepare(chunk, row):
        parts = []
        for i in range(16):
            at = (FIRST[chunk] + row) * NDEV + 8 * i
            block = xin[pl.ds(at, 8), :]
            if at == STRAIN_ROW:
                block = lanes(block, home_index)
            elif at != STRESS_ROW:
                block = lanes(block, state_index)
            parts.append(block)
        sends[chunk][pl.ds(row, NDEV, stride=CHUNKS[chunk]), :] = jnp.concatenate(parts, axis=0).T

    def prepare_chunk(chunk):
        for row in range(CHUNKS[chunk]):
            prepare(chunk, row)

    def send_chunk(chunk):
        rows = CHUNKS[chunk]
        own = pl.ds(me * rows, rows)
        for d in others(FARTHEST if chunk == LAST else SPREAD):
            pltpu.make_async_remote_copy(
                src_ref=sends[chunk].at[pl.ds(d * rows, rows)],
                dst_ref=recvs[chunk].at[own],
                send_sem=send_sem.at[chunk],
                recv_sem=recv_sem.at[chunk],
                device_id=d,
                device_id_type=LOGICAL,
            ).start()
        pltpu.make_async_copy(sends[chunk].at[own], recvs[chunk].at[own], local_sem.at[chunk]).start()

    def whole(src, dst, rows, index):
        return pltpu.make_async_remote_copy(
            src_ref=src.at[pl.ds(0, (NDEV - 1) * rows)],
            dst_ref=dst.at[pl.ds(0, (NDEV - 1) * rows)],
            send_sem=send_sem.at[index],
            recv_sem=recv_sem.at[index],
            device_id=other,
            device_id_type=LOGICAL,
        )

    for position in (0, 1):
        loads[position].wait()
    prepare_chunk(0)

    pl.semaphore_wait(barrier, NDEV - 1)

    def near(index, src, dst, dsub, drve):
        to_sub = lax.rem(sub + dsub + NSUB, NSUB)
        to_rve = lax.rem(rve + drve + NRVE, NRVE)
        return pltpu.make_async_remote_copy(
            src_ref=src,
            dst_ref=dst,
            send_sem=near_send.at[index],
            recv_sem=near_recv.at[index],
            device_id=to_sub * NRVE + to_rve,
            device_id_type=LOGICAL,
        )

    steps = ((0, 1), (1, 0), (1, 1))
    halo_in = [near(i, dtile, dhalo.at[i], -s, -r) for i, (s, r) in enumerate(steps)]
    halo_in += [near(3 + i, home_ref, home_near.at[i], s, r) for i, (s, r) in enumerate(steps)]
    for copy in halo_in:
        copy.start()
    send_chunk(0)
    loads[2].wait()
    prepare_chunk(1)
    send_chunk(1)

    for copy in halo_in:
        copy.wait()
    lane = lax.broadcasted_iota(jnp.int32, (8, NDEV), 1)
    row8 = lax.broadcasted_iota(jnp.int32, (8, NDEV), 0)
    below = jnp.where(sub < NSUB - 1, 1.0, 0.0).astype(F32)
    extended = dtile[...]
    extended = jnp.where((lane >= 16) & (lane < 24), pltpu.roll(dhalo[0], 16, axis=1), extended)
    extended = jnp.where((lane >= 24) & (lane < 40), pltpu.roll(dhalo[1], 24, axis=1) * below, extended)
    extended = jnp.where((lane >= 40) & (lane < 48), pltpu.roll(dhalo[2], 40, axis=1) * below, extended)
    slope = [jnp.zeros((8, NDEV), F32) for _ in range(3)]
    for a in range(8):
        value = lanes(extended, spread(int_ref[8 + a : 9 + a, :]))
        for k in range(3):
            slope[k] = slope[k] + float_ref[8 * k + a : 8 * k + a + 1, :] * value
    s0, s1, s2 = slope
    strains = [
        s0[0:1], s1[1:2], s2[2:3],
        s2[1:2] + s1[2:3], s2[0:1] + s0[2:3], s1[0:1] + s0[1:2],
    ]
    strain_rows = jnp.zeros((8, NDEV), F32)
    for m in range(6):
        strain_rows = jnp.where(row8 == m, spread(strains[m]), strain_rows)
    xin[pl.ds(STRAIN_ROW, 8), :] = strain_rows
    for chunk in range(MACRO, LAST):
        loads[chunk + 1].wait()
        prepare_chunk(chunk)
        send_chunk(chunk)
    xin[pl.ds(STRESS_ROW + 8, 56), :] = jnp.zeros((56, NDEV), F32)

    phase_load.wait()
    ph[pl.ds(VOX, 8), :] = jnp.zeros((8, NDEV), jnp.int32)
    inside = row8 < R
    moduli = [
        [jnp.broadcast_to(moduli_ref[which : which + 1, p : p + 1], (8, NDEV)) for p in range(3)] for which in range(2)
    ]

    @pl.loop(0, CELLS)
    def _(cell):
        label = ph[pl.ds(cell * R, 8), :]
        for which, out in ((0, lam), (1, mu)):
            value = jnp.where(
                label == 0,
                moduli[which][0],
                jnp.where(label == 1, moduli[which][1], moduli[which][2]),
            )
            out[cell] = jnp.where(inside, value, 0.0)

    av[...] = jnp.zeros((NDEV, NDEV), F32)
    up = jnp.where(row8 < 5, row8 + 1, jnp.where(row8 == 5, 0, row8))
    down = jnp.where(row8 == 0, 5, jnp.where(row8 < 6, row8 - 1, row8))

    def receive(chunk):
        rows = CHUNKS[chunk]
        own = pl.ds(me * rows, rows)
        whole(sends[chunk], recvs[chunk], rows, chunk).wait_recv()
        pltpu.make_async_copy(sends[chunk].at[own], recvs[chunk].at[own], local_sem.at[chunk]).wait()
        for row in range(rows):
            block = recvs[chunk][pl.ds(row, NDEV, stride=rows), :]
            nat[pl.ds((FIRST[chunk] + row) * NDEV, NDEV), :] = block.T

    zero = jnp.zeros((8, NDEV), F32)

    def stress_at(src, a, b, applied):
        following = (a + 1) % R
        g = []
        for i in range(3):
            here = src[i * CELLS + a * R + b]
            g.append(
                (
                    src[i * CELLS + following * R + b] - here,
                    src[i * CELLS + a * R + (b + 1) % R] - here,
                    sublanes(here, up) - here,
                )
            )
        eps = [g[0][0], g[1][1], g[2][2], g[1][2] + g[2][1], g[0][2] + g[2][0], g[0][1] + g[1][0]]
        if applied is not None:
            eps = [eps[m] + applied[m] for m in range(6)]
        cell = a * R + b
        first, second = lam[cell], mu[cell]
        volume = first * (eps[0] + eps[1] + eps[2])
        twice = second + second
        stress = [volume + twice * eps[m] for m in range(3)] + [second * eps[m] for m in range(3, 6)]
        return stress, eps

    def stresses(src, applied):
        def body(a, total):
            total = list(total)
            for b in range(R):
                stress, _ = stress_at(src, a, b, applied)
                for m in range(6):
                    sig[m * CELLS + a * R + b] = stress[m]
                    total[m] = total[m] + stress[m]
            return tuple(total)

        return sweep(body, (zero,) * 6)

    voigt = ((0, 5, 4), (5, 1, 3), (4, 3, 2))

    def force_at(src, a, b):
        before = (a + R - 1) % R
        cell = a * R + b
        here = [sig[m * CELLS + cell] for m in range(6)]
        out = []
        for i in range(3):
            total = sig[voigt[0][i] * CELLS + before * R + b] - here[voigt[0][i]]
            total = total + (sig[voigt[1][i] * CELLS + a * R + (b + R - 1) % R] - here[voigt[1][i]])
            last = here[voigt[2][i]]
            total = total + (sublanes(last, down) - last)
            out.append(total + STAB * src[i * CELLS + cell])
        return out

    def sweep(body, carry):
        for a in range(R):
            carry = body(a, carry)
        return carry

    def across(x):
        return spread(jnp.sum(x, axis=0, keepdims=True))

    def finish(case):
        alpha0, alpha1 = keep[0], keep[1]

        @pl.loop(0, R)
        def _(a):
            for i in range(3):
                to = case * CASE_ROWS + i * VOX + a * (R * R)
                for b in range(R):
                    at = i * CELLS + a * R + b
                    value = w[at] + alpha0 * p0[at] + alpha1 * p1[at]
                    new_ref[pl.ds(to + b * R, R), :] = value[0:R, :]

    for i in range(3):
        for y in range(2):
            dhalo[3, i : i + 1, 8 * y : 8 * y + 8] = load_ref[i, 0, y : y + 1, :]
    home_rows = spread(home_dev)
    grad = [float_ref[8 * k : 8 * k + 8, :] for k in range(3)]

    def to_nodes(value):
        for step in (1, 2, 4):
            value = value + pltpu.roll(value, NDEV - step, axis=1)
        value = lanes(value, int_ref[0:8, :]) * (float_ref[24:32, :] * 0.125)
        return jnp.sum(value, axis=0, keepdims=True)

    def tiled(rows):
        tile = zero
        for r, value in enumerate(rows):
            tile = jnp.where(row8 == r, spread(value), tile)
        return tile

    def residual_part():
        stress = lanes(nat[pl.ds(STRESS_ROW, 8), :], home_rows)
        rows = []
        for i in range(3):
            value = zero
            for k, m in TERMS[i]:
                value = value + grad[k] * spread(stress[m : m + 1, :])
            rows.append(to_nodes(value))
        load_rows = jnp.where((lane < 16) & (row8 < 3), dhalo[3], 0.0)
        load_square = jnp.sum(load_rows * load_rows, keepdims=True)
        part = load_rows - tiled(rows)
        first_row = part[0:1] + pltpu.roll(part[1:2], 64, axis=1)
        second_row = jnp.where(lane[0:1] == 63, jnp.broadcast_to(load_square, (1, NDEV)), part[2:3])
        return spread(first_row), spread(second_row)

    def case_body(position, carry):
        for chunk in range(CASES):

            @pl.when(position == chunk)
            def _():
                receive(chunk)

        plain = (position + 3) // 6
        case = plain * position + (1 - plain) * lax.rem(position + 1, 3)
        macro = nat[pl.ds(STRAIN_ROW, 8), :]
        applied = []
        for m in range(6):
            unit = jnp.where(case == m + 1, 1.0, 0.0).astype(F32)
            applied.append(jnp.where(position == MACRO, spread(macro[m : m + 1, :]), unit))

        start = base_of(position)
        for cell in range(CELLS):
            for i in range(3):
                w[i * CELLS + cell] = jnp.where(inside, nat[pl.ds(start + i * VOX + cell * R, 8), :], 0.0)

        total0 = stresses(w, applied)

        def first(a, rr):
            for b in range(R):
                force = force_at(w, a, b)
                for i in range(3):
                    value = -force[i]
                    p0[i * CELLS + a * R + b] = value
                    force[i] = value * value
                rr = rr + (force[0] + (force[1] + force[2]))
            return rr

        rr = across(sweep(first, zero))
        total1 = stresses(p0, None)

        def second(a, curve):
            for b in range(R):
                force = force_at(p0, a, b)
                for i in range(3):
                    ap[i * CELLS + a * R + b] = force[i]
                    force[i] = p0[i * CELLS + a * R + b] * force[i]
                curve = curve + (force[0] + (force[1] + force[2]))
            return curve

        alpha0 = rr / across(sweep(second, zero))

        def reduce(a, total):
            total = list(total)
            for j in range(3 * R):
                at = a * (3 * R) + j
                value = p0[at] - alpha0 * ap[at]
                p1[at] = value
                total[j % 6] = total[j % 6] + value * value
            return tuple(total)

        parts = sweep(reduce, (zero,) * 6)
        rn = across(((parts[0] + parts[1]) + (parts[2] + parts[3])) + (parts[4] + parts[5]))
        beta = rn / rr

        for at in range(3 * CELLS):
            p1[at] = p1[at] + beta * p0[at]

        def third(a, carried):
            curve, total = carried[0], list(carried[1:])
            for b in range(R):
                stress, eps = stress_at(p1, a, b, None)
                for m in range(6):
                    total[m] = total[m] + stress[m]
                work = [stress[m] * eps[m] for m in range(6)]
                here = [p1[i * CELLS + a * R + b] for i in range(3)]
                kept = STAB * ((here[0] * here[0] + here[1] * here[1]) + here[2] * here[2])
                curve = curve + (((work[0] + work[1]) + (work[2] + work[3])) + ((work[4] + work[5]) + kept))
            return (curve, *total)

        found = sweep(third, (zero,) * 7)
        alpha1 = rn / across(found[0])
        for m in range(6):
            mean = jnp.sum(total0[m] + alpha0 * total1[m] + alpha1 * found[1 + m], axis=0, keepdims=True)
            av[pl.ds(case * 6 + m, 1), :] = mean * (1.0 / VOX)

        keep[0], keep[1] = alpha0, alpha1

        @pl.when(position < LAST)
        def _():
            finish(case)

        @pl.when(position == MACRO)
        def _():
            xin[pl.ds(STRESS_ROW, 8), :] = av[0:8, :]
            prepare_chunk(LAST)
            send_chunk(LAST)

        return carry

    lax.fori_loop(0, CASES, case_body, 0)

    for r, (m, j) in enumerate(ENTRIES):
        entry = av[(1 + j) * 6 + m : (1 + j) * 6 + m + 1, :]
        if m != j:
            entry = entry + av[(1 + m) * 6 + j : (1 + m) * 6 + j + 1, :]
        spare[r : r + 1, :] = entry
    spare[15:16, :] = jnp.zeros((1, NDEV), F32)
    step_back = lax.rem(lane + 3, 4) - lax.rem(lane, 4) + lane
    here = [spare[0:8, :], spare[8:16, :]]
    beside = [lanes(x, step_back) for x in here]
    under = [pltpu.roll(x, NRVE, axis=1) for x in here + beside]
    back_rows = jnp.concatenate([zero] * 8 + here + beside + under, axis=0).T
    first_row, second_row = residual_part()
    for block in range(16):
        rows_out[pl.ds(block * 16, 8, stride=2), :] = first_row
        rows_out[pl.ds(block * 16 + 1, 8, stride=2), :] = back_rows[8 * block : 8 * block + 8, :] + second_row
    own = pl.ds(me * 2, 2)
    for d in others(FARTHEST):
        pltpu.make_async_remote_copy(
            src_ref=rows_out.at[pl.ds(d * 2, 2)],
            dst_ref=rows_in.at[own],
            send_sem=send_sem.at[RESULT],
            recv_sem=recv_sem.at[RESULT],
            device_id=d,
            device_id_type=LOGICAL,
        ).start()
    own_copy = pltpu.make_async_copy(rows_out.at[own], rows_in.at[own], local_sem.at[RESULT])
    own_copy.start()
    finish(ORDER[LAST])
    whole(rows_out, rows_in, 2, RESULT).wait_recv()
    own_copy.wait()
    back = rows_in[pl.ds(1, NDEV, stride=2), :].T
    above = jnp.where(sub > 0, 1.0, 0.0).astype(F32)
    targets = [home_rows] + [spread(lax.shift_right_logical(home_near[b], 7)) for b in range(3)]
    product = {(k, l): grad[k] * grad[l] for k in range(3) for l in range(k, 3)}
    parts = []
    for b in range(4):
        found = [lanes(back[64 + 16 * b + 8 * h : 64 + 16 * b + 8 * h + 8, :], targets[b]) for h in range(2)]
        values = []
        for i in range(3):
            value = zero
            for (k, m), (l, j) in itertools.combinations_with_replacement(TERMS[i], 2):
                r = ENTRIES.index((min(m, j), max(m, j)))
                value = value + product[min(k, l), max(k, l)] * spread(found[r // 8][r % 8 : r % 8 + 1, :])
            values.append(value)
        parts.append(values)
    lower = row8 < 4
    crossing = (lax.rem(row8, 4) >= 2) & (lane >= 64)
    diagonal = []
    for i in range(3):
        inner = jnp.where(lower, parts[0][i], parts[2][i] * above)
        outer = jnp.where(lower, parts[1][i], parts[3][i] * above)
        value = jnp.where(crossing, outer, inner)
        for step in (1, 2, 4):
            value = value + pltpu.roll(value, NDEV - step, axis=1)
        value = lanes(value, int_ref[16:24, :]) * 0.125
        diagonal.append(jnp.sum(value, axis=0, keepdims=True))
    node = tiled(diagonal)

    turn = jnp.where(lax.rem(row8, 4) == 0, row8 + 3, row8 - 1)
    square = zero
    load_sum = zero
    low = lax.rem(lane, 64)
    for half in range(2):
        before_z = zero
        for block in range(16):
            value = rows_in[pl.ds(block * 16 + half, 8, stride=2), :]
            if half == 1:
                load_sum = load_sum + jnp.where(lane == 63, value, 0.0)
                value = jnp.where(lane < 48, value, 0.0)
            before = pltpu.roll(sublanes(value, turn), NDEV - 16, axis=1)
            value = value + jnp.where((low < 8) | ((low >= 24) & (low < 32)), before, 0.0)
            plane = pltpu.roll(value, NDEV - 24, axis=1)
            shifted = jnp.where(row8 < 4, pltpu.roll(before_z, 4, axis=0), pltpu.roll(plane, 4, axis=0))
            before_z = plane
            value = jnp.where(low < 16, value + shifted, 0.0)
            whole_residual[half, pl.ds(block * 8, 8), :] = value
            square = square + value * value
    ratio = jnp.sqrt(jnp.sum(square, keepdims=True) / jnp.sum(load_sum, keepdims=True))
    norm_ref[...] = jnp.broadcast_to(ratio, (8, NDEV))

    pair = whole_residual[0, pl.ds(me, 1), :]
    residual = jnp.concatenate([pair, pltpu.roll(pair, 64, axis=1), whole_residual[1, pl.ds(me, 1), :]], axis=0)
    moved = dtile[0:3, :] + residual / jnp.maximum(node[0:3], FLOOR)
    for i in range(3):
        for y in range(2):
            displaced_ref[i, 0, y : y + 1, :] = moved[i : i + 1, 8 * y : 8 * y + 8]
            residual_ref[i, 0, y : y + 1, :] = residual[i : i + 1, 8 * y : 8 * y + 8]

    for chunk in range(CASES):
        whole(sends[chunk], recvs[chunk], CHUNKS[chunk], chunk).wait_send()
    whole(rows_out, rows_in, 2, RESULT).wait_send()


def write_out(new_vmem, displaced_vmem, residual_vmem, norm_vmem, new_ref, displaced_ref, residual_ref, norm_ref, sem):
    copies = []
    for case in range(CASES):
        span = pl.ds(case * CASE_ROWS, CASE_ROWS)
        copies.append((new_vmem.at[span], new_ref.at[span]))
    copies += [(displaced_vmem, displaced_ref), (residual_vmem, residual_ref), (norm_vmem.at[pl.ds(0, 1)], norm_ref)]
    copies = [pltpu.make_async_copy(src, dst, sem.at[i]) for i, (src, dst) in enumerate(copies)]
    for copy in copies:
        copy.start()
    for copy in copies:
        copy.wait()


def per_device(displacement, load, home_slot, micro_state, state_slot, phases, phase_moduli):
    floats, ints = tables()
    vmem = pl.BlockSpec(memory_space=pltpu.VMEM)
    hbm = pl.BlockSpec(memory_space=pltpu.HBM)
    buffers = [pltpu.VMEM((NDEV * rows, NDEV), F32) for rows in CHUNKS]
    cells = pltpu.VMEM((3 * CELLS, 8, NDEV), F32)
    dma = pltpu.SemaphoreType.DMA
    arguments = (
        displacement,
        load,
        home_slot.reshape(1, NDEV),
        state_slot.reshape(1, NDEV),
        phase_moduli,
        jnp.asarray(floats),
        jnp.asarray(ints),
        micro_state.reshape(ROWS, NDEV),
        phases,
    )
    results = pl.pallas_call(
        kernel,
        out_shape=(
            pltpu.VMEM((ROWS, NDEV), F32),
            pltpu.VMEM(displacement.shape, F32),
            pltpu.VMEM(displacement.shape, F32),
            pltpu.VMEM((8, NDEV), F32),
        ),
        in_specs=[hbm] * 9,
        out_specs=(vmem,) * 4,
        scratch_shapes=[
            pltpu.VMEM(displacement.shape, F32),
            pltpu.VMEM(load.shape, F32),
            pltpu.VMEM((1, NDEV), jnp.int32),
            pltpu.VMEM((1, NDEV), jnp.int32),
            pltpu.VMEM(phase_moduli.shape, F32),
            pltpu.VMEM(floats.shape, F32),
            pltpu.VMEM(ints.shape, jnp.int32),
            pltpu.VMEM((ROWS + 72, NDEV), F32),
            pltpu.VMEM((VOX + 8, NDEV), jnp.int32),
            *buffers,
            *buffers,
            pltpu.VMEM((ROWS + 72, NDEV), F32),
            pltpu.VMEM((CELLS, 8, NDEV), F32),
            pltpu.VMEM((CELLS, 8, NDEV), F32),
            cells,
            cells,
            cells,
            cells,
            pltpu.VMEM((6 * CELLS, 8, NDEV), F32),
            pltpu.VMEM((2, 8, NDEV), F32),
            pltpu.VMEM((NDEV, NDEV), F32),
            pltpu.VMEM((2 * NDEV, NDEV), F32),
            pltpu.VMEM((2 * NDEV, NDEV), F32),
            pltpu.VMEM((8, NDEV), F32),
            pltpu.VMEM((4, 8, NDEV), F32),
            pltpu.VMEM((3, 1, NDEV), jnp.int32),
            pltpu.VMEM((16, NDEV), F32),
            pltpu.VMEM((2, NDEV, NDEV), F32),
            dma((7,)),
            dma((CASES,)),
            dma,
            dma((CASES + 1,)),
            dma((CASES + 1,)),
            dma((CASES + 1,)),
            dma((6,)),
            dma((6,)),
        ],
        compiler_params=pltpu.CompilerParams(
            collective_id=1, has_side_effects=True, vmem_limit_bytes=48 * 1024 * 1024
        ),
    )(*[pltpu.with_memory_space_constraint(x, pltpu.HBM) for x in arguments])
    new_state, displaced, residual, norm = pl.pallas_call(
        write_out,
        out_shape=tuple(pltpu.HBM(shape, F32) for shape in (results[0].shape, *[displacement.shape] * 2, (1, NDEV))),
        in_specs=[vmem] * 4,
        out_specs=(hbm,) * 4,
        scratch_shapes=[dma((CASES + 3,))],
        compiler_params=pltpu.CompilerParams(vmem_limit_bytes=4 * 1024 * 1024),
    )(*results)
    return new_state.reshape(CASES, 3, VOX, NDEV), displaced, residual, norm[0, 0]


def solution(mesh):
    both = ("sub", "rve")
    return jax.shard_map(
        per_device,
        mesh=mesh,
        in_specs=(
            P(None, "sub", "rve", None),
            P(None, "sub", "rve", None),
            P(both),
            P(None, None, None, both),
            P(both),
            P(None, both),
            P(),
        ),
        out_specs=(
            P(None, None, None, both),
            P(None, "sub", "rve", None),
            P(None, "sub", "rve", None),
            P(),
        ),
        check_vma=False,
    )
```

```python
import itertools
import math

import jax
import jax.numpy as jnp
import numpy as np
from jax import lax
from jax.experimental import pallas as pl
from jax.experimental.pallas import tpu as pltpu
from jax.sharding import PartitionSpec as P

R = 6
VOX = 216
CASES = 7
STAB = 0.1
FLOOR = 1.0
NDEV = 128
NRVE = 4
NSUB = 32
ROWS = CASES * 3 * VOX
CASE_ROWS = 3 * VOX
CHUNKS = (6, 5, 5, 5, 5, 5, 5)
FIRST = (0, 6, 11, 16, 21, 26, 31)
LAST = len(CHUNKS) - 1
ORDER = (1, 2, 0, 3, 4, 5, 6)
MACRO = 2
STRAIN_ROW = 3 * CASE_ROWS
STRESS_ROW = 7 * CASE_ROWS + 8
RESULT = LAST + 1
CELLS = 36
LOGICAL = pl.DeviceIdType.LOGICAL
F32 = jnp.float32
TERMS = (((0, 0), (2, 4), (1, 5)), ((1, 1), (2, 3), (0, 5)), ((2, 2), (1, 3), (0, 4)))
ENTRIES = [(m, m) for m in range(6)]
ENTRIES += [(min(t[0][1], t[1][1]), max(t[0][1], t[1][1])) for i in range(3) for t in itertools.combinations(TERMS[i], 2)]


def tables():
    offset = 0.5 / math.sqrt(3.0)
    places = (0.5 - offset, 0.5 + offset)
    slopes = np.zeros((3, 8, NDEV), np.float32)
    for g in range(NDEV):
        q = g % 8
        at = (places[q % 2], places[q // 2 % 2], places[q // 4])
        for a in range(8):
            bits = (a % 2, a // 2 % 2, a // 4)
            w = [at[k] if bits[k] else 1.0 - at[k] for k in range(3)]
            s = [1.0 if bits[k] else -1.0 for k in range(3)]
            slopes[0, a, g] = s[0] * w[1] * w[2]
            slopes[1, a, g] = w[0] * s[1] * w[2]
            slopes[2, a, g] = w[0] * w[1] * s[2]
    mask = np.zeros((8, NDEV), np.float32)
    pick = np.zeros((8, NDEV), np.int32)
    for n in range(48):
        nz, ny, nx = n // 24, n // 8 % 3, n % 8
        for a in range(8):
            ax, ay, az = a % 2, a // 2 % 2, a // 4
            ly = ny - ay
            if az == nz and 0 <= ly < 2:
                mask[a, n] = 1.0
                pick[a, n] = (ly * 8 + (nx - ax) % 8) * 8
    corner = np.zeros((8, NDEV), np.int32)
    for g in range(NDEV):
        ly, ex = g // 64, g // 8 % 8
        for a in range(8):
            ax, ay, az = a % 2, a // 2 % 2, a // 4
            corner[a, g] = az * 24 + (ly + ay) * 8 + (ex + ax) % 8
    own = np.zeros((8, NDEV), np.int32)
    for n in range(16):
        ny, nx = n // 8, n % 8
        for a in range(8):
            ax, ay = a % 2, a // 2 % 2
            own[a, n] = ((1 - ny if ay else ny) * 8 + (nx - ax) % 8) * 8
    floats = np.concatenate([slopes.reshape(24, NDEV), mask], axis=0)
    ints = np.concatenate([pick, corner, own], axis=0)
    return floats, ints


def base_of(position):
    return position * CASE_ROWS + 8 * ((position + 3) // 6)


def around(step):
    return min(step, 4 - step)


SPREAD = [((i // 16 + i) % 4, (i // 4 + i) % 4, c, i % 4) for c in range(2) for i in range(64)][1:]
FARTHEST = sorted(SPREAD, key=lambda o: -(around(o[0]) + around(o[1]) + around(o[3]) + 0.3 * o[2]))


def lanes(x, index):
    return jnp.take_along_axis(x, index, axis=1, mode="promise_in_bounds")


def sublanes(x, index):
    return jnp.take_along_axis(x, index, axis=0, mode="promise_in_bounds")


def spread(row):
    return jnp.broadcast_to(row, (8, NDEV))


def inverse(target):
    column = jnp.broadcast_to(target, (NDEV, NDEV)).T
    lane = lax.broadcasted_iota(jnp.int32, (NDEV, NDEV), 1)
    row = lax.broadcasted_iota(jnp.int32, (NDEV, NDEV), 0)
    return jnp.sum(jnp.where(column == lane, row, 0).astype(F32), axis=0, keepdims=True).astype(jnp.int32)


def kernel(
    disp_hbm, load_hbm, home_hbm, state_hbm, moduli_hbm, float_hbm, int_hbm, micro_ref, phase_ref,
    new_ref, displaced_ref, residual_ref, norm_ref,
    disp_ref, load_ref, home_ref, state_slot_ref, moduli_ref, float_ref, int_ref, xin, ph, send0, send1, send2, send3, send4, send5, send6, recv0, recv1, recv2, recv3, recv4, recv5, recv6,
    nat, lam, mu, w, p0, p1, ap, sig, keep, av, rows_out, rows_in, dtile, dhalo, home_near, spare, whole_residual,
    small_sem, in_sem, ph_sem, local_sem, send_sem, recv_sem, near_send, near_recv,
):
    sub, rve = lax.axis_index("sub"), lax.axis_index("rve")
    me = sub * NRVE + rve
    sends = (send0, send1, send2, send3, send4, send5, send6)
    recvs = (recv0, recv1, recv2, recv3, recv4, recv5, recv6)
    along_z = [lax.rem(sub // 8 + i, 4) * 32 for i in range(4)]
    along_y = [lax.rem(lax.rem(sub // 2, 4) + i, 4) * 8 for i in range(4)]
    along_c = [lax.rem(lax.rem(sub, 2) + i, 2) * 4 for i in range(2)]
    along_x = [lax.rem(rve + i, 4) for i in range(4)]

    def others(order):
        for z, y, c, x in order:
            yield along_z[z] + along_y[y] + (along_c[c] + along_x[x])

    other = along_z[0] + along_y[0] + (along_c[0] + along_x[1])

    barrier = pltpu.get_barrier_semaphore()

    for d in others(FARTHEST):
        pl.semaphore_signal(barrier, inc=1, device_id=d, device_id_type=LOGICAL)

    small = []
    pairs = (
        (state_hbm, state_slot_ref), (home_hbm, home_ref), (disp_hbm, disp_ref), (load_hbm, load_ref),
        (moduli_hbm, moduli_ref), (float_hbm, float_ref), (int_hbm, int_ref),
    )
    for i, (src, dst) in enumerate(pairs):
        small.append(pltpu.make_async_copy(src, dst, small_sem.at[i]))
        small[-1].start()

    loads = []
    for position, case in enumerate(ORDER):
        copy = pltpu.make_async_copy(
            micro_ref.at[pl.ds(case * CASE_ROWS, CASE_ROWS)],
            xin.at[pl.ds(base_of(position), CASE_ROWS)],
            in_sem.at[position],
        )
        copy.start()
        loads.append(copy)
    phase_load = pltpu.make_async_copy(phase_ref, ph.at[pl.ds(0, VOX)], ph_sem)
    phase_load.start()

    for copy in small:
        copy.wait()
    dtile[...] = jnp.zeros((8, NDEV), F32)
    for i in range(3):
        for y in range(2):
            dtile[i : i + 1, 8 * y : 8 * y + 8] = disp_ref[i, 0, y : y + 1, :]

    home_dev = lax.shift_right_logical(home_ref[...], 7)
    state_index = spread(inverse(lax.shift_right_logical(state_slot_ref[...], 7)))
    home_index = spread(inverse(home_dev))

    def prepare(chunk, row):
        parts = []
        for i in range(16):
            at = (FIRST[chunk] + row) * NDEV + 8 * i
            block = xin[pl.ds(at, 8), :]
            if at == STRAIN_ROW:
                block = lanes(block, home_index)
            elif at != STRESS_ROW:
                block = lanes(block, state_index)
            parts.append(block)
        sends[chunk][pl.ds(row, NDEV, stride=CHUNKS[chunk]), :] = jnp.concatenate(parts, axis=0).T

    def prepare_chunk(chunk):
        for row in range(CHUNKS[chunk]):
            prepare(chunk, row)

    def send_chunk(chunk):
        rows = CHUNKS[chunk]
        own = pl.ds(me * rows, rows)
        for d in others(FARTHEST if chunk == LAST else SPREAD):
            pltpu.make_async_remote_copy(
                src_ref=sends[chunk].at[pl.ds(d * rows, rows)],
                dst_ref=recvs[chunk].at[own],
                send_sem=send_sem.at[chunk],
                recv_sem=recv_sem.at[chunk],
                device_id=d,
                device_id_type=LOGICAL,
            ).start()
        pltpu.make_async_copy(sends[chunk].at[own], recvs[chunk].at[own], local_sem.at[chunk]).start()

    def whole(src, dst, rows, index):
        return pltpu.make_async_remote_copy(
            src_ref=src.at[pl.ds(0, (NDEV - 1) * rows)],
            dst_ref=dst.at[pl.ds(0, (NDEV - 1) * rows)],
            send_sem=send_sem.at[index],
            recv_sem=recv_sem.at[index],
            device_id=other,
            device_id_type=LOGICAL,
        )

    for position in (0, 1):
        loads[position].wait()
    prepare_chunk(0)

    pl.semaphore_wait(barrier, NDEV - 1)

    def near(index, src, dst, dsub, drve):
        to_sub = lax.rem(sub + dsub + NSUB, NSUB)
        to_rve = lax.rem(rve + drve + NRVE, NRVE)
        return pltpu.make_async_remote_copy(
            src_ref=src,
            dst_ref=dst,
            send_sem=near_send.at[index],
            recv_sem=near_recv.at[index],
            device_id=to_sub * NRVE + to_rve,
            device_id_type=LOGICAL,
        )

    steps = ((0, 1), (1, 0), (1, 1))
    halo_in = [near(i, dtile, dhalo.at[i], -s, -r) for i, (s, r) in enumerate(steps)]
    halo_in += [near(3 + i, home_ref, home_near.at[i], s, r) for i, (s, r) in enumerate(steps)]
    for copy in halo_in:
        copy.start()
    send_chunk(0)
    loads[2].wait()
    prepare_chunk(1)
    send_chunk(1)

    for copy in halo_in:
        copy.wait()
    lane = lax.broadcasted_iota(jnp.int32, (8, NDEV), 1)
    row8 = lax.broadcasted_iota(jnp.int32, (8, NDEV), 0)
    below = jnp.where(sub < NSUB - 1, 1.0, 0.0).astype(F32)
    extended = dtile[...]
    extended = jnp.where((lane >= 16) & (lane < 24), pltpu.roll(dhalo[0], 16, axis=1), extended)
    extended = jnp.where((lane >= 24) & (lane < 40), pltpu.roll(dhalo[1], 24, axis=1) * below, extended)
    extended = jnp.where((lane >= 40) & (lane < 48), pltpu.roll(dhalo[2], 40, axis=1) * below, extended)
    slope = [jnp.zeros((8, NDEV), F32) for _ in range(3)]
    for a in range(8):
        value = lanes(extended, spread(int_ref[8 + a : 9 + a, :]))
        for k in range(3):
            slope[k] = slope[k] + float_ref[8 * k + a : 8 * k + a + 1, :] * value
    s0, s1, s2 = slope
    strains = [
        s0[0:1], s1[1:2], s2[2:3],
        s2[1:2] + s1[2:3], s2[0:1] + s0[2:3], s1[0:1] + s0[1:2],
    ]
    strain_rows = jnp.zeros((8, NDEV), F32)
    for m in range(6):
        strain_rows = jnp.where(row8 == m, spread(strains[m]), strain_rows)
    xin[pl.ds(STRAIN_ROW, 8), :] = strain_rows
    for chunk in range(MACRO, LAST):
        loads[chunk + 1].wait()
        prepare_chunk(chunk)
        send_chunk(chunk)
    xin[pl.ds(STRESS_ROW + 8, 56), :] = jnp.zeros((56, NDEV), F32)

    phase_load.wait()
    ph[pl.ds(VOX, 8), :] = jnp.zeros((8, NDEV), jnp.int32)
    inside = row8 < R
    moduli = [
        [jnp.broadcast_to(moduli_ref[which : which + 1, p : p + 1], (8, NDEV)) for p in range(3)] for which in range(2)
    ]

    @pl.loop(0, CELLS)
    def _(cell):
        label = ph[pl.ds(cell * R, 8), :]
        for which, out in ((0, lam), (1, mu)):
            value = jnp.where(
                label == 0,
                moduli[which][0],
                jnp.where(label == 1, moduli[which][1], moduli[which][2]),
            )
            out[cell] = jnp.where(inside, value, 0.0)

    av[...] = jnp.zeros((NDEV, NDEV), F32)
    up = jnp.where(row8 < 5, row8 + 1, jnp.where(row8 == 5, 0, row8))
    down = jnp.where(row8 == 0, 5, jnp.where(row8 < 6, row8 - 1, row8))

    def receive(chunk):
        rows = CHUNKS[chunk]
        own = pl.ds(me * rows, rows)
        whole(sends[chunk], recvs[chunk], rows, chunk).wait_recv()
        pltpu.make_async_copy(sends[chunk].at[own], recvs[chunk].at[own], local_sem.at[chunk]).wait()
        for row in range(rows):
            block = recvs[chunk][pl.ds(row, NDEV, stride=rows), :]
            nat[pl.ds((FIRST[chunk] + row) * NDEV, NDEV), :] = block.T

    zero = jnp.zeros((8, NDEV), F32)

    def stress_at(src, a, b, applied):
        following = (a + 1) % R
        g = []
        for i in range(3):
            here = src[i * CELLS + a * R + b]
            g.append(
                (
                    src[i * CELLS + following * R + b] - here,
                    src[i * CELLS + a * R + (b + 1) % R] - here,
                    sublanes(here, up) - here,
                )
            )
        eps = [g[0][0], g[1][1], g[2][2], g[1][2] + g[2][1], g[0][2] + g[2][0], g[0][1] + g[1][0]]
        if applied is not None:
            eps = [eps[m] + applied[m] for m in range(6)]
        cell = a * R + b
        first, second = lam[cell], mu[cell]
        volume = first * (eps[0] + eps[1] + eps[2])
        twice = second + second
        stress = [volume + twice * eps[m] for m in range(3)] + [second * eps[m] for m in range(3, 6)]
        return stress, eps

    def stresses(src, applied):
        def body(a, total):
            total = list(total)
            for b in range(R):
                stress, _ = stress_at(src, a, b, applied)
                for m in range(6):
                    sig[m * CELLS + a * R + b] = stress[m]
                    total[m] = total[m] + stress[m]
            return tuple(total)

        return sweep(body, (zero,) * 6)

    voigt = ((0, 5, 4), (5, 1, 3), (4, 3, 2))

    def force_at(src, a, b):
        before = (a + R - 1) % R
        cell = a * R + b
        here = [sig[m * CELLS + cell] for m in range(6)]
        out = []
        for i in range(3):
            total = sig[voigt[0][i] * CELLS + before * R + b] - here[voigt[0][i]]
            total = total + (sig[voigt[1][i] * CELLS + a * R + (b + R - 1) % R] - here[voigt[1][i]])
            last = here[voigt[2][i]]
            total = total + (sublanes(last, down) - last)
            out.append(total + STAB * src[i * CELLS + cell])
        return out

    def sweep(body, carry):
        for a in range(R):
            carry = body(a, carry)
        return carry

    def across(x):
        return spread(jnp.sum(x, axis=0, keepdims=True))

    def finish(case):
        alpha0, alpha1 = keep[0], keep[1]

        @pl.loop(0, R)
        def _(a):
            for i in range(3):
                to = case * CASE_ROWS + i * VOX + a * (R * R)
                for b in range(R):
                    at = i * CELLS + a * R + b
                    value = w[at] + alpha0 * p0[at] + alpha1 * p1[at]
                    new_ref[pl.ds(to + b * R, R), :] = value[0:R, :]

    for i in range(3):
        for y in range(2):
            dhalo[3, i : i + 1, 8 * y : 8 * y + 8] = load_ref[i, 0, y : y + 1, :]
    home_rows = spread(home_dev)
    grad = [float_ref[8 * k : 8 * k + 8, :] for k in range(3)]

    def to_nodes(value):
        for step in (1, 2, 4):
            value = value + pltpu.roll(value, NDEV - step, axis=1)
        value = lanes(value, int_ref[0:8, :]) * (float_ref[24:32, :] * 0.125)
        return jnp.sum(value, axis=0, keepdims=True)

    def tiled(rows):
        tile = zero
        for r, value in enumerate(rows):
            tile = jnp.where(row8 == r, spread(value), tile)
        return tile

    def residual_part():
        stress = lanes(nat[pl.ds(STRESS_ROW, 8), :], home_rows)
        rows = []
        for i in range(3):
            value = zero
            for k, m in TERMS[i]:
                value = value + grad[k] * spread(stress[m : m + 1, :])
            rows.append(to_nodes(value))
        load_rows = jnp.where((lane < 16) & (row8 < 3), dhalo[3], 0.0)
        load_square = jnp.sum(load_rows * load_rows, keepdims=True)
        part = load_rows - tiled(rows)
        first_row = part[0:1] + pltpu.roll(part[1:2], 64, axis=1)
        second_row = jnp.where(lane[0:1] == 63, jnp.broadcast_to(load_square, (1, NDEV)), part[2:3])
        return spread(first_row), spread(second_row)

    def case_body(position, carry):
        for chunk in range(CASES):

            @pl.when(position == chunk)
            def _():
                receive(chunk)

        plain = (position + 3) // 6
        case = plain * position + (1 - plain) * lax.rem(position + 1, 3)
        macro = nat[pl.ds(STRAIN_ROW, 8), :]
        applied = []
        for m in range(6):
            unit = jnp.where(case == m + 1, 1.0, 0.0).astype(F32)
            applied.append(jnp.where(position == MACRO, spread(macro[m : m + 1, :]), unit))

        start = base_of(position)
        for cell in range(CELLS):
            for i in range(3):
                w[i * CELLS + cell] = jnp.where(inside, nat[pl.ds(start + i * VOX + cell * R, 8), :], 0.0)

        keep[2], keep[3] = residual_part()
        total0 = stresses(w, applied)

        def first(a, rr):
            for b in range(R):
                force = force_at(w, a, b)
                for i in range(3):
                    value = -force[i]
                    p0[i * CELLS + a * R + b] = value
                    force[i] = value * value
                rr = rr + (force[0] + (force[1] + force[2]))
            return rr

        rr = across(sweep(first, zero))
        total1 = stresses(p0, None)

        def second(a, curve):
            for b in range(R):
                force = force_at(p0, a, b)
                for i in range(3):
                    ap[i * CELLS + a * R + b] = force[i]
                    force[i] = p0[i * CELLS + a * R + b] * force[i]
                curve = curve + (force[0] + (force[1] + force[2]))
            return curve

        alpha0 = rr / across(sweep(second, zero))

        def reduce(a, total):
            total = list(total)
            for j in range(3 * R):
                at = a * (3 * R) + j
                value = p0[at] - alpha0 * ap[at]
                p1[at] = value
                total[j % 6] = total[j % 6] + value * value
            return tuple(total)

        parts = sweep(reduce, (zero,) * 6)
        rn = across(((parts[0] + parts[1]) + (parts[2] + parts[3])) + (parts[4] + parts[5]))
        beta = rn / rr

        for at in range(3 * CELLS):
            p1[at] = p1[at] + beta * p0[at]

        def third(a, carried):
            curve, total = carried[0], list(carried[1:])
            for b in range(R):
                stress, eps = stress_at(p1, a, b, None)
                for m in range(6):
                    total[m] = total[m] + stress[m]
                work = [stress[m] * eps[m] for m in range(6)]
                here = [p1[i * CELLS + a * R + b] for i in range(3)]
                kept = STAB * ((here[0] * here[0] + here[1] * here[1]) + here[2] * here[2])
                curve = curve + (((work[0] + work[1]) + (work[2] + work[3])) + ((work[4] + work[5]) + kept))
            return (curve, *total)

        found = sweep(third, (zero,) * 7)
        alpha1 = rn / across(found[0])
        for m in range(6):
            mean = jnp.sum(total0[m] + alpha0 * total1[m] + alpha1 * found[1 + m], axis=0, keepdims=True)
            av[pl.ds(case * 6 + m, 1), :] = mean * (1.0 / VOX)

        keep[0], keep[1] = alpha0, alpha1

        @pl.when(position < LAST)
        def _():
            finish(case)

        @pl.when(position == MACRO)
        def _():
            xin[pl.ds(STRESS_ROW, 8), :] = av[0:8, :]
            prepare_chunk(LAST)
            send_chunk(LAST)

        return carry

    lax.fori_loop(0, CASES, case_body, 0)

    for r, (m, j) in enumerate(ENTRIES):
        entry = av[(1 + j) * 6 + m : (1 + j) * 6 + m + 1, :]
        if m != j:
            entry = entry + av[(1 + m) * 6 + j : (1 + m) * 6 + j + 1, :]
        spare[r : r + 1, :] = entry
    spare[15:16, :] = jnp.zeros((1, NDEV), F32)
    step_back = lax.rem(lane + 3, 4) - lax.rem(lane, 4) + lane
    here = [spare[0:8, :], spare[8:16, :]]
    beside = [lanes(x, step_back) for x in here]
    under = [pltpu.roll(x, NRVE, axis=1) for x in here + beside]
    back_rows = jnp.concatenate([zero] * 8 + here + beside + under, axis=0).T
    first_row, second_row = keep[2], keep[3]
    for block in range(16):
        rows_out[pl.ds(block * 16, 8, stride=2), :] = first_row
        rows_out[pl.ds(block * 16 + 1, 8, stride=2), :] = back_rows[8 * block : 8 * block + 8, :] + second_row
    own = pl.ds(me * 2, 2)
    for d in others(FARTHEST):
        pltpu.make_async_remote_copy(
            src_ref=rows_out.at[pl.ds(d * 2, 2)],
            dst_ref=rows_in.at[own],
            send_sem=send_sem.at[RESULT],
            recv_sem=recv_sem.at[RESULT],
            device_id=d,
            device_id_type=LOGICAL,
        ).start()
    own_copy = pltpu.make_async_copy(rows_out.at[own], rows_in.at[own], local_sem.at[RESULT])
    own_copy.start()
    finish(ORDER[LAST])
    whole(rows_out, rows_in, 2, RESULT).wait_recv()
    own_copy.wait()
    back = rows_in[pl.ds(1, NDEV, stride=2), :].T
    above = jnp.where(sub > 0, 1.0, 0.0).astype(F32)
    targets = [home_rows] + [spread(lax.shift_right_logical(home_near[b], 7)) for b in range(3)]
    product = {(k, l): grad[k] * grad[l] for k in range(3) for l in range(k, 3)}
    parts = []
    for b in range(4):
        found = [lanes(back[64 + 16 * b + 8 * h : 64 + 16 * b + 8 * h + 8, :], targets[b]) for h in range(2)]
        values = []
        for i in range(3):
            value = zero
            for (k, m), (l, j) in itertools.combinations_with_replacement(TERMS[i], 2):
                r = ENTRIES.index((min(m, j), max(m, j)))
                value = value + product[min(k, l), max(k, l)] * spread(found[r // 8][r % 8 : r % 8 + 1, :])
            values.append(value)
        parts.append(values)
    lower = row8 < 4
    crossing = (lax.rem(row8, 4) >= 2) & (lane >= 64)
    diagonal = []
    for i in range(3):
        inner = jnp.where(lower, parts[0][i], parts[2][i] * above)
        outer = jnp.where(lower, parts[1][i], parts[3][i] * above)
        value = jnp.where(crossing, outer, inner)
        points = [lanes(value, int_ref[16:24, :] + q) for q in range(8)]
        while len(points) > 1:
            points = [x + y for x, y in zip(points[::2], points[1::2])]
        diagonal.append(jnp.sum(points[0] * 0.125, axis=0, keepdims=True))
    node = tiled(diagonal)

    turn = jnp.where(lax.rem(row8, 4) == 0, row8 + 3, row8 - 1)
    square = zero
    load_sum = zero
    low = lax.rem(lane, 64)
    for half in range(2):
        before_z = zero
        for block in range(16):
            value = rows_in[pl.ds(block * 16 + half, 8, stride=2), :]
            if half == 1:
                load_sum = load_sum + jnp.where(lane == 63, value, 0.0)
                value = jnp.where(lane < 48, value, 0.0)
            before = pltpu.roll(sublanes(value, turn), NDEV - 16, axis=1)
            value = value + jnp.where((low < 8) | ((low >= 24) & (low < 32)), before, 0.0)
            plane = pltpu.roll(value, NDEV - 24, axis=1)
            shifted = jnp.where(row8 < 4, pltpu.roll(before_z, 4, axis=0), pltpu.roll(plane, 4, axis=0))
            before_z = plane
            value = jnp.where(low < 16, value + shifted, 0.0)
            whole_residual[half, pl.ds(block * 8, 8), :] = value
            square = square + value * value
    ratio = jnp.sqrt(jnp.sum(square, keepdims=True) / jnp.sum(load_sum, keepdims=True))
    norm_ref[...] = jnp.broadcast_to(ratio, (8, NDEV))

    pair = whole_residual[0, pl.ds(me, 1), :]
    residual = jnp.concatenate([pair, pltpu.roll(pair, 64, axis=1), whole_residual[1, pl.ds(me, 1), :]], axis=0)
    moved = dtile[0:3, :] + residual / jnp.maximum(node[0:3], FLOOR)
    for i in range(3):
        for y in range(2):
            displaced_ref[i, 0, y : y + 1, :] = moved[i : i + 1, 8 * y : 8 * y + 8]
            residual_ref[i, 0, y : y + 1, :] = residual[i : i + 1, 8 * y : 8 * y + 8]

    for chunk in range(CASES):
        whole(sends[chunk], recvs[chunk], CHUNKS[chunk], chunk).wait_send()
    whole(rows_out, rows_in, 2, RESULT).wait_send()


def write_out(new_vmem, displaced_vmem, residual_vmem, norm_vmem, new_ref, displaced_ref, residual_ref, norm_ref, sem):
    copies = []
    for case in range(CASES):
        span = pl.ds(case * CASE_ROWS, CASE_ROWS)
        copies.append((new_vmem.at[span], new_ref.at[span]))
    copies += [(displaced_vmem, displaced_ref), (residual_vmem, residual_ref), (norm_vmem.at[pl.ds(0, 1)], norm_ref)]
    copies = [pltpu.make_async_copy(src, dst, sem.at[i]) for i, (src, dst) in enumerate(copies)]
    for copy in copies:
        copy.start()
    for copy in copies:
        copy.wait()


def per_device(displacement, load, home_slot, micro_state, state_slot, phases, phase_moduli):
    floats, ints = tables()
    vmem = pl.BlockSpec(memory_space=pltpu.VMEM)
    hbm = pl.BlockSpec(memory_space=pltpu.HBM)
    buffers = [pltpu.VMEM((NDEV * rows, NDEV), F32) for rows in CHUNKS]
    cells = pltpu.VMEM((3 * CELLS, 8, NDEV), F32)
    dma = pltpu.SemaphoreType.DMA
    arguments = (
        displacement,
        load,
        home_slot.reshape(1, NDEV),
        state_slot.reshape(1, NDEV),
        phase_moduli,
        jnp.asarray(floats),
        jnp.asarray(ints),
        micro_state.reshape(ROWS, NDEV),
        phases,
    )
    results = pl.pallas_call(
        kernel,
        out_shape=(
            pltpu.VMEM((ROWS, NDEV), F32),
            pltpu.VMEM(displacement.shape, F32),
            pltpu.VMEM(displacement.shape, F32),
            pltpu.VMEM((8, NDEV), F32),
        ),
        in_specs=[hbm] * 9,
        out_specs=(vmem,) * 4,
        scratch_shapes=[
            pltpu.VMEM(displacement.shape, F32),
            pltpu.VMEM(load.shape, F32),
            pltpu.VMEM((1, NDEV), jnp.int32),
            pltpu.VMEM((1, NDEV), jnp.int32),
            pltpu.VMEM(phase_moduli.shape, F32),
            pltpu.VMEM(floats.shape, F32),
            pltpu.VMEM(ints.shape, jnp.int32),
            pltpu.VMEM((ROWS + 72, NDEV), F32),
            pltpu.VMEM((VOX + 8, NDEV), jnp.int32),
            *buffers,
            *buffers,
            pltpu.VMEM((ROWS + 72, NDEV), F32),
            pltpu.VMEM((CELLS, 8, NDEV), F32),
            pltpu.VMEM((CELLS, 8, NDEV), F32),
            cells,
            cells,
            cells,
            cells,
            pltpu.VMEM((6 * CELLS, 8, NDEV), F32),
            pltpu.VMEM((4, 8, NDEV), F32),
            pltpu.VMEM((NDEV, NDEV), F32),
            pltpu.VMEM((2 * NDEV, NDEV), F32),
            pltpu.VMEM((2 * NDEV, NDEV), F32),
            pltpu.VMEM((8, NDEV), F32),
            pltpu.VMEM((4, 8, NDEV), F32),
            pltpu.VMEM((3, 1, NDEV), jnp.int32),
            pltpu.VMEM((16, NDEV), F32),
            pltpu.VMEM((2, NDEV, NDEV), F32),
            dma((7,)),
            dma((CASES,)),
            dma,
            dma((CASES + 1,)),
            dma((CASES + 1,)),
            dma((CASES + 1,)),
            dma((6,)),
            dma((6,)),
        ],
        compiler_params=pltpu.CompilerParams(
            collective_id=1, has_side_effects=True, vmem_limit_bytes=48 * 1024 * 1024
        ),
    )(*[pltpu.with_memory_space_constraint(x, pltpu.HBM) for x in arguments])
    new_state, displaced, residual, norm = pl.pallas_call(
        write_out,
        out_shape=tuple(pltpu.HBM(shape, F32) for shape in (results[0].shape, *[displacement.shape] * 2, (1, NDEV))),
        in_specs=[vmem] * 4,
        out_specs=(hbm,) * 4,
        scratch_shapes=[dma((CASES + 3,))],
        compiler_params=pltpu.CompilerParams(vmem_limit_bytes=4 * 1024 * 1024),
    )(*results)
    return new_state.reshape(CASES, 3, VOX, NDEV), displaced, residual, norm[0, 0]


def solution(mesh):
    both = ("sub", "rve")
    return jax.shard_map(
        per_device,
        mesh=mesh,
        in_specs=(
            P(None, "sub", "rve", None),
            P(None, "sub", "rve", None),
            P(both),
            P(None, None, None, both),
            P(both),
            P(None, both),
            P(),
        ),
        out_specs=(
            P(None, None, None, both),
            P(None, "sub", "rve", None),
            P(None, "sub", "rve", None),
            P(),
        ),
        check_vma=False,
    )
```
